32 devices in a mesh: dp: 1 (over z), fsdp: 32 (over y, x, core).
Axes of the slice: x: 4, y: 4, z: 1, core: 2. Of those that a mesh axis runs over, the one named last changes fastest.
The devices are a block of a 4x4x8 slice.
Arguments:
- tokens: bfloat16 [64, 64, 4096], P(('dp', 'fsdp'))
- k_cache: bfloat16 [64, 4096, 8, 128], P(('dp', 'fsdp'))
- v_cache: bfloat16 [64, 4096, 8, 128], P(('dp', 'fsdp'))
- prefix_len: int32 [64], P(('dp', 'fsdp'))
- rope_cos: float32 [64, 64, 64], P(('dp', 'fsdp'))
- rope_sin: float32 [64, 64, 64], P(('dp', 'fsdp'))
- norm_attn: bfloat16 [4096], P('fsdp')
- w_qkv: bfloat16 [4096, 6144], P('fsdp')
- b_qkv: bfloat16 [6144], P('fsdp')
- sink_logits: float32 [32], replicated
- w_out: bfloat16 [4096, 4096], P('fsdp')
- b_out: bfloat16 [4096], P('fsdp')
- norm_router: bfloat16 [4096], P('fsdp')
- w_router: bfloat16 [4096, 8], P('fsdp')
- b_router: float32 [8], replicated
Outputs:
- output 1: bfloat16 [64, 64, 4096], P(('dp', 'fsdp'))
- output 2: float32 [64, 64, 8], P(('dp', 'fsdp'))
- output 3: bfloat16 [64, 64, 8, 128], P(('dp', 'fsdp'))
- output 4: bfloat16 [64, 64, 8, 128], P(('dp', 'fsdp'))
All inputs are finite; a program needn't handle non-finite values.
Results may differ from the reference program's by a relative error of at most 0.00187.
Values are sent between devices in bfloat16 or wider.
A program may use at most 768 MiB of HBM per device.

```python
import math
import jax
import jax.numpy as jnp
from jax import lax

REQUESTS = 64
NEW_TOKENS = 64
CACHE_LEN = 4096
MODEL_DIM = 4096
Q_HEADS = 32
KV_HEADS = 8
HEAD_DIM = 128
EXPERTS = 8
QKV_WIDTH = (Q_HEADS + 2 * KV_HEADS) * HEAD_DIM
Q_WIDTH = Q_HEADS * HEAD_DIM
NORM_EPS = 1e-5
ROPE_BASE = 150000.0


def rope_tables(lengths):
    half_dim = HEAD_DIM // 2
    inv_freq = jnp.power(ROPE_BASE, -2.0 * jnp.arange(half_dim, dtype=jnp.float32) / HEAD_DIM)
    positions = lengths.astype(jnp.float32)[:, None] + jnp.arange(NEW_TOKENS, dtype=jnp.float32)[None, :]
    angles = positions[:, :, None] * inv_freq[None, None, :]
    return jnp.cos(angles), jnp.sin(angles)


def draw_lengths(key):
    sub_keys = jax.random.split(key, 3)
    lengths = jax.random.randint(sub_keys[0], (REQUESTS,), 0, CACHE_LEN + 1)
    full_slot = jax.random.randint(sub_keys[1], (), 0, REQUESTS)
    empty_slot = (full_slot + 1 + jax.random.randint(sub_keys[2], (), 0, REQUESTS - 1)) % REQUESTS
    slot_ids = jnp.arange(REQUESTS)
    lengths = jnp.where(slot_ids == full_slot, CACHE_LEN, lengths)
    lengths = jnp.where(slot_ids == empty_slot, 0, lengths)
    return lengths.astype(jnp.int32)


def normal_draw(key, shape):
    return jax.random.normal(key, shape, jnp.float32)


def setup_inputs(seed: int = 0, part: int = 0) -> dict:
    base_key = jax.random.key(seed)
    part_keys = jax.random.split(jax.random.fold_in(base_key, part), 4)
    weight_keys = jax.random.split(jax.random.fold_in(base_key, 1000003), 10)
    lengths = draw_lengths(part_keys[0])
    rope_cos, rope_sin = rope_tables(lengths)
    tokens = normal_draw(part_keys[1], (REQUESTS, NEW_TOKENS, MODEL_DIM))
    k_cache = 1.5 * normal_draw(part_keys[2], (REQUESTS, CACHE_LEN, KV_HEADS, HEAD_DIM))
    v_cache = normal_draw(part_keys[3], (REQUESTS, CACHE_LEN, KV_HEADS, HEAD_DIM))
    return {
        'tokens': tokens.astype(jnp.bfloat16),
        'k_cache': k_cache.astype(jnp.bfloat16),
        'v_cache': v_cache.astype(jnp.bfloat16),
        'prefix_len': lengths,
        'rope_cos': rope_cos,
        'rope_sin': rope_sin,
        'norm_attn': (1.0 + 0.2 * normal_draw(weight_keys[0], (MODEL_DIM,))).astype(jnp.bfloat16),
        'w_qkv': (normal_draw(weight_keys[1], (MODEL_DIM, QKV_WIDTH)) * (1.5 / math.sqrt(MODEL_DIM))).astype(jnp.bfloat16),
        'b_qkv': (0.3 * normal_draw(weight_keys[2], (QKV_WIDTH,))).astype(jnp.bfloat16),
        'sink_logits': math.log(CACHE_LEN) + 1.0 + 2.0 * normal_draw(weight_keys[3], (Q_HEADS,)),
        'w_out': (normal_draw(weight_keys[4], (Q_WIDTH, MODEL_DIM)) * (2.5 / math.sqrt(Q_WIDTH))).astype(jnp.bfloat16),
        'b_out': (0.3 * normal_draw(weight_keys[5], (MODEL_DIM,))).astype(jnp.bfloat16),
        'norm_router': (1.0 + 0.2 * normal_draw(weight_keys[6], (MODEL_DIM,))).astype(jnp.bfloat16),
        'w_router': (normal_draw(weight_keys[7], (MODEL_DIM, EXPERTS)) * (1.0 / math.sqrt(MODEL_DIM))).astype(jnp.bfloat16),
        'b_router': 0.5 * normal_draw(weight_keys[8], (EXPERTS,)),
    }


def rms_scale(values, gain_vec):
    val_f32 = values.astype(jnp.float32)
    inv_rms = lax.rsqrt(jnp.mean(val_f32 * val_f32, axis=-1, keepdims=True) + NORM_EPS)
    return (val_f32 * inv_rms * gain_vec.astype(jnp.float32)).astype(jnp.bfloat16)


def apply_rope(values, cos_tab, sin_tab):
    half_dim = values.shape[-1] // 2
    first_half = values[..., :half_dim]
    second_half = values[..., half_dim:]
    return jnp.concatenate([first_half * cos_tab - second_half * sin_tab, second_half * cos_tab + first_half * sin_tab], axis=-1)


def attend_one(q_block, k_prev, v_prev, k_cur, v_cur, prev_len, head_sinks):
    n_new, n_kv, n_group, head_dim = q_block.shape
    n_prev = k_prev.shape[0]
    score_scale = head_dim ** -0.5
    q_f32 = q_block.astype(jnp.float32)
    s_prev = jnp.einsum('ckgd,pkd->kgcp', q_f32, k_prev.astype(jnp.float32)) * score_scale
    s_cur = jnp.einsum('ckgd,jkd->kgcj', q_f32, k_cur.astype(jnp.float32)) * score_scale
    s_prev = jnp.where(jnp.arange(n_prev) < prev_len, s_prev, -1e30)
    s_cur = jnp.where(jnp.arange(n_new)[None, :] <= jnp.arange(n_new)[:, None], s_cur, -1e30)
    sink_col = head_sinks.astype(jnp.float32).reshape(n_kv, n_group, 1, 1)
    row_max = jnp.maximum(jnp.maximum(jnp.max(s_prev, axis=-1, keepdims=True), jnp.max(s_cur, axis=-1, keepdims=True)), sink_col)
    p_prev = jnp.exp(s_prev - row_max)
    p_cur = jnp.exp(s_cur - row_max)
    denominator = jnp.sum(p_prev, axis=-1) + jnp.sum(p_cur, axis=-1) + jnp.exp(sink_col - row_max)[..., 0]
    weighted = jnp.einsum('kgcp,pkd->ckgd', p_prev.astype(jnp.bfloat16).astype(jnp.float32), v_prev.astype(jnp.float32)) + jnp.einsum('kgcj,jkd->ckgd', p_cur.astype(jnp.bfloat16).astype(jnp.float32), v_cur.astype(jnp.float32))
    return (weighted / jnp.transpose(denominator, (2, 0, 1))[..., None]).astype(jnp.bfloat16)


def reference(tokens, k_cache, v_cache, prefix_len, rope_cos, rope_sin, norm_attn, w_qkv, b_qkv, sink_logits, w_out, b_out, norm_router, w_router, b_router):
    n_req, n_new, model_dim = tokens.shape
    n_kv = k_cache.shape[2]
    head_dim = k_cache.shape[3]
    n_heads = sink_logits.shape[0]
    n_tok = n_req * n_new
    q_width = n_heads * head_dim
    kv_width = n_kv * head_dim
    flat_tok = tokens.reshape(n_tok, model_dim)
    qkv_rows = jnp.dot(rms_scale(flat_tok, norm_attn), w_qkv, preferred_element_type=jnp.float32) + b_qkv.astype(jnp.float32)
    cos_tab = rope_cos.reshape(n_tok, 1, head_dim // 2)
    sin_tab = rope_sin.reshape(n_tok, 1, head_dim // 2)
    q_rot = apply_rope(qkv_rows[:, :q_width].reshape(n_tok, n_heads, head_dim), cos_tab, sin_tab).astype(jnp.bfloat16)
    k_rot = apply_rope(qkv_rows[:, q_width:q_width + kv_width].reshape(n_tok, n_kv, head_dim), cos_tab, sin_tab).astype(jnp.bfloat16)
    v_rows = qkv_rows[:, q_width + kv_width:].astype(jnp.bfloat16)
    q_req = q_rot.reshape(n_req, n_new, n_kv, n_heads // n_kv, head_dim)
    k_req = k_rot.reshape(n_req, n_new, n_kv, head_dim)
    v_req = v_rows.reshape(n_req, n_new, n_kv, head_dim)
    attn_out = lax.map(lambda item_tuple: attend_one(item_tuple[0], item_tuple[1], item_tuple[2], item_tuple[3], item_tuple[4], item_tuple[5], sink_logits), (q_req, k_cache, v_cache, k_req, v_req, prefix_len))
    attn_flat = attn_out.reshape(n_tok, q_width)
    proj_out = jnp.dot(attn_flat, w_out, preferred_element_type=jnp.float32) + b_out.astype(jnp.float32)
    new_resid = (flat_tok.astype(jnp.float32) + proj_out).astype(jnp.bfloat16)
    logits = jnp.dot(rms_scale(new_resid, norm_router), w_router, preferred_element_type=jnp.float32) + b_router.astype(jnp.float32)
    return (new_resid.reshape(n_req, n_new, model_dim), logits.reshape(n_req, n_new, -1), k_req, v_req)
```

```python
import functools
import math

import jax
import jax.numpy as jnp
from jax import lax
from jax.experimental import pallas as pl
from jax.experimental.pallas import tpu as pltpu
from jax.sharding import PartitionSpec as P

NORM_EPS = 1e-5
AXIS = 'fsdp'
CORES = 2
MESH_ID = pl.DeviceIdType.MESH
BF16 = jnp.bfloat16
F32 = jnp.float32
LOG2E = 1.4426950408889634


class Place:
    def __init__(self, side):
        index = lax.axis_index(AXIS)
        self.side = side
        self.row = side * CORES
        self.c = lax.rem(index, CORES)
        self.x = lax.rem(index // CORES, side)
        self.y = index // self.row
        self.j = self.x * CORES + self.c

    def spot(self, dx, other=False):
        core = (1 - self.c) if other else self.c
        return lax.rem(self.x + dx, self.side) * CORES + core

    def line(self, dy):
        return lax.rem(self.y + dy, self.side)

    def mate(self, spot):
        return self.y * self.row + spot

    def above(self, dy):
        return self.line(dy) * self.row + self.j


class Sends:
    def __init__(self):
        self.started = []

    def __call__(self, src, dst, send_sem, recv_sem, device):
        copy = pltpu.make_async_remote_copy(
            src_ref=src, dst_ref=dst, send_sem=send_sem, recv_sem=recv_sem,
            device_id={AXIS: device}, device_id_type=MESH_ID)
        copy.start()
        self.started.append(copy)

    def finish(self):
        for copy in self.started:
            copy.wait_send()


def landed(ref, sem):
    pltpu.make_async_copy(ref, ref, sem).wait()


def meet(place):
    barrier = pltpu.get_barrier_semaphore()
    peers = [place.mate(place.spot(dx, other)) for dx in range(place.side) for other in (False, True) if dx or other]
    peers += [place.above(1), place.above(place.side - 1)]
    for peer in peers:
        pl.semaphore_signal(barrier, inc=1, device_id={AXIS: peer}, device_id_type=MESH_ID)
    pl.semaphore_wait(barrier, len(peers))


def rel_order(side):
    return [(0, True), (1, False), (side - 1, False), (1, True), (side - 1, True), (2, False), (2, True)]


class RowGather:
    def __init__(self, place, sends, buf, ring_s, ring_r, pair_s, pair_r):
        self.p, self.sends, self.buf = place, sends, buf
        self.ring_s, self.ring_r, self.pair_s, self.pair_r = ring_s, ring_r, pair_s, pair_r
        self.half = buf.shape[1] // 2

    def view(self, spot, h):
        return self.buf.at[spot, pl.ds(h * self.half, self.half)]

    def ring(self, spot, h, slot, dx):
        v = self.view(spot, h)
        self.sends(v, v, self.ring_s.at[slot], self.ring_r.at[slot], self.p.mate(self.p.spot(dx)))

    def pair(self, dx, h):
        v = self.view(self.p.spot(dx), h)
        slot = dx * 2 + h
        self.sends(v, v, self.pair_s.at[slot], self.pair_r.at[slot], self.p.mate(self.p.spot(0, True)))

    def start(self):
        p, back = self.p, self.p.side - 1
        self.ring(p.spot(0), 0, 0, 1)
        self.ring(p.spot(0), 1, 2, back)
        self.pair(0, 0)
        self.pair(0, 1)
        self.ring(p.spot(0), 1, 1, 1)
        self.ring(p.spot(0), 0, 3, back)

    def first(self):
        p, back = self.p, self.p.side - 1
        landed(self.view(p.spot(back), 0), self.ring_r.at[0])
        self.ring(p.spot(back), 0, 4, 1)
        self.pair(back, 0)
        landed(self.view(p.spot(1), 1), self.ring_r.at[2])
        self.ring(p.spot(1), 1, 5, back)
        self.pair(1, 1)

    def second(self):
        p, back = self.p, self.p.side - 1
        landed(self.view(p.spot(back), 1), self.ring_r.at[1])
        self.pair(back, 1)
        landed(self.view(p.spot(1), 0), self.ring_r.at[3])
        self.pair(1, 0)

    def third(self):
        p = self.p
        landed(self.view(p.spot(2), 0), self.ring_r.at[4])
        self.pair(2, 0)
        landed(self.view(p.spot(2), 1), self.ring_r.at[5])
        self.pair(2, 1)

    def from_pair(self, dx):
        for h in range(2):
            landed(self.view(self.p.spot(dx, True), h), self.pair_r.at[dx * 2 + h])


class ColumnGather:
    def __init__(self, place, sends, buf, up_s, up_r, down_s, down_r, far_s, far_r):
        self.p, self.sends, self.buf = place, sends, buf
        self.up_s, self.up_r, self.down_s, self.down_r = up_s, up_r, down_s, down_r
        self.far_s, self.far_r = far_s, far_r
        self.order = [(0, False)] + rel_order(place.side)

    def own(self, k):
        p = self.p
        v = self.buf.at[p.y, p.spot(*self.order[k])]
        self.sends(v, v, self.up_s.at[k], self.up_r.at[k], p.above(1))
        self.sends(v, v, self.down_s.at[k], self.down_r.at[k], p.above(p.side - 1))

    def near(self, k):
        p, back = self.p, self.p.side - 1
        spot = p.spot(*self.order[k])
        low, high = self.buf.at[p.line(back), spot], self.buf.at[p.line(1), spot]
        landed(low, self.up_r.at[k])
        if k % 2 == 0:
            self.sends(low, low, self.far_s.at[k], self.far_r.at[k], p.above(1))
        landed(high, self.down_r.at[k])
        if k % 2 == 1:
            self.sends(high, high, self.far_s.at[k], self.far_r.at[k], p.above(back))

    def far(self, k):
        p = self.p
        landed(self.buf.at[p.line(2), p.spot(*self.order[k])], self.far_r.at[k])


def dot_nt(a, b):
    return lax.dot_general(a, b, (((1,), (1,)), ((), ())), preferred_element_type=F32)


def project_kernel(side, heads, kv, w_ref, wo_ref, x_ref, cs_ref, pack_ref,
                   qkv_out, xb_out, pack_out, wo_out,
                   wl, wol, wq, xa, hh, csa, packs, acc, res, xbs,
                   s_wl, s_wol, s_loc, s_a2a, r_a2a, s_o, r_o, s_cs, r_cs, s_pk, r_pk, s_pv, r_pv,
                   s_ring, r_ring, s_pair, r_pair, s_up, r_up, s_dn, r_dn, s_far, r_far, s_res, r_res):
    p = Place(side)
    row = p.row
    back = side - 1
    head = w_ref.shape[1] // (heads + 2 * kv)
    qw = heads // kv * head
    depth = w_ref.shape[0]
    wide = qw + 2 * head
    rel = rel_order(side)
    sends = Sends()

    def take(spot, dst, sem):
        parts = ((spot * qw, qw, 0), (heads * head + spot * head, head, qw),
                 ((heads + kv) * head + spot * head, head, qw + head))
        for start, size, at in parts:
            pltpu.make_async_copy(w_ref.at[:, pl.ds(pl.multiple_of(start, head), size)],
                                  dst.at[:, pl.ds(at, size)], sem).start()

    take(p.j, wq.at[p.y, p.j], s_wl.at[0])
    for k, at in enumerate(rel):
        take(p.spot(*at), wl.at[k], s_wl.at[k + 1])
    pltpu.make_async_copy(x_ref, xa.at[p.j], s_loc.at[0]).start()
    ow = wol.shape[-1]
    for k, at in enumerate(rel):
        pltpu.make_async_copy(wo_ref.at[:, pl.ds(pl.multiple_of(p.spot(*at) * ow, head), ow)], wol.at[k],
                              s_wol.at[k]).start()
    own_o = pltpu.make_async_copy(wo_ref.at[:, pl.ds(pl.multiple_of(p.j * ow, head), ow)], wol.at[row - 1],
                                  s_wol.at[row - 1])
    own_o.start()
    packs[p.y, p.j] = pack_ref[...]
    csa[p.j] = cs_ref[...]

    meet(p)

    gather = ColumnGather(p, sends, wq, s_up, r_up, s_dn, r_dn, s_far, r_far)
    tokens = RowGather(p, sends, xa, s_ring, r_ring, s_pair, r_pair)
    landed(wq.at[p.y, p.j], s_wl.at[0])
    gather.own(0)
    for k, at in enumerate(rel):
        sends(pack_ref, packs.at[p.y, p.j], s_pk.at[k], r_pk.at[k], p.mate(p.spot(*at)))
    for k, at in enumerate(rel):
        landed(wl.at[k], s_wl.at[k + 1])
        sends(wl.at[k], wq.at[p.y, p.j], s_a2a.at[k], r_a2a.at[k], p.mate(p.spot(*at)))
    for k, at in enumerate(rel):
        sends(cs_ref, csa.at[p.j], s_cs.at[k], r_cs.at[k], p.mate(p.spot(*at)))
    landed(xa.at[p.j], s_loc.at[0])
    tokens.start()
    for k, at in enumerate(rel):
        landed(wol.at[k], s_wol.at[k])
        sends(wol.at[k], wo_out.at[p.j], s_o.at[k], r_o.at[k], p.mate(p.spot(*at)))
    own_o.wait()
    pltpu.make_async_copy(wol.at[row - 1], wo_out.at[p.j], s_loc.at[1]).start()

    def source(at):
        return p.spot(lax.rem(side - at[0], side) if at[0] else 0, at[1])

    def mirror(k):
        dx, other = rel[k]
        return rel.index(((side - dx) % side, other))

    for k in range(row - 1):
        landed(packs.at[p.y, p.spot(*rel[mirror(k)])], r_pk.at[k])
    pv = packs.at[p.y]
    sends(pv, pv, s_pv.at[0], r_pv.at[0], p.above(1))
    sends(pv, pv, s_pv.at[1], r_pv.at[1], p.above(back))
    for k in range(row - 1):
        m = mirror(k)
        landed(wq.at[p.y, p.spot(*rel[k])], r_a2a.at[m])
        gather.own(k + 1)
    pu = packs.at[p.line(back)]
    landed(pu, r_pv.at[0])
    sends(pu, pu, s_pv.at[2], r_pv.at[2], p.above(1))
    landed(packs.at[p.line(1)], r_pv.at[1])
    landed(packs.at[p.line(2)], r_pv.at[2])
    for k in range(row - 1):
        landed(csa.at[p.spot(*rel[mirror(k)])], r_cs.at[k])
    pltpu.make_async_copy(packs, pack_out, s_loc.at[2]).start()

    model = xa.shape[-1]
    xw = xbs.shape[-1]

    def norm(spot):
        xbs[spot] = xa[spot, :, pl.ds(pl.multiple_of(p.j * xw, head), xw)]
        total = jnp.zeros((xa.shape[1], head), F32)
        for i in range(model // head):
            v = xa[spot, :, i * head:(i + 1) * head].astype(F32)
            total = total + v * v
        inv = lax.rsqrt(jnp.sum(total, axis=-1, keepdims=True) / model + NORM_EPS)
        for i in range(model // head):
            v = xa[spot, :, i * head:(i + 1) * head].astype(F32)
            g = packs[i // row, i % row, 0:1, :]
            hh[spot, :, i * head:(i + 1) * head] = (v * inv * g).astype(BF16)

    span = row * depth

    def part(dx, dy):
        chip = lax.rem(p.x + dx, side)
        rows = hh[pl.ds(chip * CORES, CORES), :, pl.ds(pl.multiple_of(p.line(dy) * span, span), span)]
        rows = rows.reshape(CORES * hh.shape[1], span)
        return jnp.dot(rows, wq[p.line(dy)].reshape(span, wide), preferred_element_type=F32)

    def bias(m):
        e, k = m // 3, lax.rem(m, 3)
        out = 0.0
        for c in range(CORES):
            d = e * CORES + c
            out = out + packs[d // row, lax.rem(d, row), pl.ds(3 + k, 1), :]
        return out

    lanes = lax.broadcasted_iota(jnp.int32, (1, head), 1)

    def finish(dx):
        total = acc[dx] + part(dx, 2)
        chip = lax.rem(p.x + dx, side)
        cs = csa[pl.ds(chip * CORES, CORES)].reshape(CORES * csa.shape[1], head)
        turned = pltpu.roll(cs, head // 2, 1)
        low = lanes < head // 2
        cos = jnp.where(low, cs, turned)
        sin = jnp.where(low, -turned, cs)
        n_q = heads // kv
        for i in range(n_q + 2):
            m = p.j * n_q + i if i < n_q else (heads + p.j if i == n_q else heads + kv + p.j)
            t = total[:, i * head:(i + 1) * head] + bias(m)
            if i <= n_q:
                t = t * cos + pltpu.roll(t, head // 2, 1) * sin
            res[dx * CORES:(dx + 1) * CORES, :, i * head:(i + 1) * head] = t.astype(BF16).reshape(CORES, -1, head)
        for c in range(CORES):
            spot = chip * CORES + c
            src = res.at[dx * CORES + c]
            if dx:
                sends(src, qkv_out.at[p.j], s_res.at[dx * CORES + c], r_res.at[p.j], p.mate(spot))
            else:
                @pl.when(p.c == c)
                def _():
                    pltpu.make_async_copy(src, qkv_out.at[p.j], r_res.at[p.j]).start()

                @pl.when(p.c != c)
                def _():
                    pltpu.make_async_remote_copy(
                        src_ref=src, dst_ref=qkv_out.at[p.j], send_sem=s_res.at[0], recv_sem=r_res.at[p.j],
                        device_id={AXIS: p.mate(spot)}, device_id_type=MESH_ID).start()

    norm(p.spot(0))
    tokens.from_pair(0)
    norm(p.spot(0, True))
    tokens.first()
    for k in range(0, 4):
        gather.near(k)
    acc[0] = part(0, 0)
    tokens.second()
    for k in range(4, row):
        gather.near(k)
    acc[0] += part(0, 1)
    acc[0] += part(0, back)
    for dx in (back, 1):
        norm(p.spot(dx))
        tokens.from_pair(dx)
        norm(p.spot(dx, True))
        acc[dx] = part(dx, 0)
        acc[dx] += part(dx, 1)
        acc[dx] += part(dx, back)
    tokens.third()
    norm(p.spot(2))
    tokens.from_pair(2)
    norm(p.spot(2, True))
    xb = pltpu.make_async_copy(xbs, xb_out, s_loc.at[3])
    xb.start()
    for k in range(row):
        gather.far(k)
    finish(1)
    finish(back)
    acc[2] = part(2, 0)
    acc[2] += part(2, 1)
    acc[2] += part(2, back)
    finish(2)
    finish(0)
    for k in range(row - 1):
        landed(wo_out.at[p.spot(*rel[mirror(k)])], r_o.at[k])
    for i in range(row):
        landed(qkv_out.at[i], r_res.at[i])
    landed(wo_out.at[p.j], s_loc.at[1])
    landed(packs, s_loc.at[2])
    xb.wait()
    landed(res.at[0], s_res.at[0])
    sends.finish()


def attend_kernel(kv, len_ref, sink_ref, qkv_ref, k_ref, v_ref, o_ref, kb, vb, kt, vt, acc, top, low, s_k, s_v):
    n_req = k_ref.shape[0]
    head = k_ref.shape[-1]
    new = qkv_ref.shape[1] // n_req
    group = qkv_ref.shape[2] // head - 2
    block = kb.shape[1]
    scale = head ** -0.5 * LOG2E
    rows = group * new

    def span(r):
        return pl.ds(pl.multiple_of(r * new, new), new)

    def query(r, i):
        return jnp.concatenate([qkv_ref[i, span(r), g * head:(g + 1) * head] for g in range(group)], axis=0)

    def request(r, carry):
        length = len_ref[r]
        count = (length + block - 1) // block

        def fetch(b, slot):
            return (pltpu.make_async_copy(k_ref.at[r, pl.ds(b * block, block)], kb.at[slot], s_k.at[slot]),
                    pltpu.make_async_copy(v_ref.at[r, pl.ds(b * block, block)], vb.at[slot], s_v.at[slot]))

        @pl.when(count > 0)
        def _():
            for copy in fetch(0, 0):
                copy.start()

        causal = (lax.rem(lax.broadcasted_iota(jnp.int32, (rows, new), 0), new)
                  >= lax.broadcasted_iota(jnp.int32, (rows, new), 1))
        for i in range(kv):
            k_new = qkv_ref[i, span(r), group * head:(group + 1) * head]
            v_new = qkv_ref[i, span(r), (group + 1) * head:]
            s = jnp.where(causal, dot_nt(query(r, i), k_new) * scale, -1e30)
            sink = jnp.concatenate([jnp.full((new, head), sink_ref[i * group + g] * LOG2E, F32) for g in range(group)], axis=0)
            m = jnp.maximum(jnp.max(s, axis=-1, keepdims=True), sink)
            pr = jnp.exp2(s - m[:, :1])
            low[i] = jnp.sum(pr, axis=-1, keepdims=True) + jnp.exp2(sink - m)
            top[i] = m
            acc[i] = jnp.dot(pr.astype(BF16), v_new, preferred_element_type=F32)

        def step(b, _):
            slot = lax.rem(b, 2)

            @pl.when(b + 1 < count)
            def _():
                for copy in fetch(b + 1, 1 - slot):
                    copy.start()

            for copy in fetch(b, slot):
                copy.wait()
            kt[...] = pltpu.einshape('skd->ksd', kb[slot])
            vt[...] = pltpu.einshape('skd->ksd', vb[slot])
            limit = length - b * block

            def heads(masked):
                for i in range(kv):
                    s = dot_nt(query(r, i), kt[i]) * scale
                    if masked:
                        s = jnp.where(lax.broadcasted_iota(jnp.int32, (1, block), 1) < limit, s, -1e30)
                    m_old = top[i]
                    m = jnp.maximum(m_old, jnp.max(s, axis=-1, keepdims=True))
                    pr = jnp.exp2(s - m[:, :1])
                    fade = jnp.exp2(m_old - m)
                    low[i] = low[i] * fade + jnp.sum(pr, axis=-1, keepdims=True)
                    top[i] = m
                    acc[i] = acc[i] * fade + jnp.dot(pr.astype(BF16), vt[i], preferred_element_type=F32)

            @pl.when(limit >= block)
            def _():
                heads(False)

            @pl.when(limit < block)
            def _():
                heads(True)
            return 0

        lax.fori_loop(0, count, step, 0)
        for i in range(kv):
            out = (acc[i] / low[i]).astype(BF16)
            for g in range(group):
                at = (i * group + g) * head
                o_ref[span(r), at:at + head] = out[g * new:(g + 1) * new]
        return carry

    lax.fori_loop(0, n_req, request, 0)


def output_kernel(side, experts, o_ref, wo_ref, xb_ref, packs, br_ref, resid_out, logit_out,
                  oa, wq, xbv, acc, res, own,
                  s_loc, s_ring, r_ring, s_pair, r_pair, s_up, r_up, s_dn, r_dn, s_far, r_far, s_res, r_res):
    p = Place(side)
    row = p.row
    back = side - 1
    head = packs.shape[-1]
    depth = wq.shape[2]
    wide = wq.shape[3]
    sends = Sends()
    loads = [pltpu.make_async_copy(wo_ref, wq.at[p.y], s_loc.at[0]),
             pltpu.make_async_copy(o_ref, oa.at[p.j], s_loc.at[1]),
             pltpu.make_async_copy(xb_ref, xbv, s_loc.at[2])]
    for copy in loads:
        copy.start()
    meet(p)
    gather = ColumnGather(p, sends, wq, s_up, r_up, s_dn, r_dn, s_far, r_far)
    tokens = RowGather(p, sends, oa, s_ring, r_ring, s_pair, r_pair)
    loads[1].wait()
    tokens.start()
    loads[0].wait()
    for k in range(row):
        gather.own(k)
    loads[2].wait()
    span = row * depth

    def part(dx, dy):
        chip = lax.rem(p.x + dx, side)
        rows = oa[pl.ds(chip * CORES, CORES), :, pl.ds(pl.multiple_of(p.line(dy) * span, span), span)]
        rows = rows.reshape(CORES * oa.shape[1], span)
        return jnp.dot(rows, wq[p.line(dy)].reshape(span, wide), preferred_element_type=F32)

    def finish(dx):
        total = acc[dx] + part(dx, 2)
        chip = lax.rem(p.x + dx, side)
        for i in range(wide // head):
            d = p.j * (wide // head) + i
            b = packs[d // row, lax.rem(d, row), 1:2, :]
            at = pl.ds(i * head, head)
            base = xbv[pl.ds(chip * CORES, CORES), :, at].reshape(-1, head).astype(F32)
            t = base + (total[:, i * head:(i + 1) * head] + b)
            res[dx * CORES:(dx + 1) * CORES, :, at] = t.astype(BF16).reshape(CORES, -1, head)
        for c in range(CORES):
            spot = chip * CORES + c
            src = res.at[dx * CORES + c]
            if dx:
                sends(src, own.at[p.j], s_res.at[dx * CORES + c], r_res.at[p.j], p.mate(spot))
            else:
                @pl.when(p.c == c)
                def _():
                    own[p.j] = src[...]

                @pl.when(p.c != c)
                def _():
                    pltpu.make_async_remote_copy(
                        src_ref=src, dst_ref=own.at[p.j], send_sem=s_res.at[0], recv_sem=r_res.at[p.j],
                        device_id={AXIS: p.mate(spot)}, device_id_type=MESH_ID).start()

    tokens.from_pair(0)
    acc[0] = part(0, 0)
    tokens.first()
    for k in range(0, 4):
        gather.near(k)
    tokens.second()
    for k in range(4, row):
        gather.near(k)
    acc[0] += part(0, 1)
    acc[0] += part(0, back)
    for dx in (back, 1):
        tokens.from_pair(dx)
        acc[dx] = part(dx, 0)
        acc[dx] += part(dx, 1)
        acc[dx] += part(dx, back)
    tokens.third()
    for k in range(row):
        gather.far(k)
    finish(1)
    finish(back)
    tokens.from_pair(2)
    acc[2] = part(2, 0)
    acc[2] += part(2, 1)
    acc[2] += part(2, back)
    finish(2)
    finish(0)
    for dx, other in rel_order(side):
        spot = p.spot(dx, other)
        landed(own.at[spot], r_res.at[spot])
    n_tok = own.shape[1]
    model = row * wide
    outs = []
    for i in range(row):
        copy = pltpu.make_async_copy(own.at[i], resid_out.at[:, pl.ds(i * wide, wide)], s_loc.at[3 + i])
        copy.start()
        outs.append(copy)
    total = jnp.zeros((n_tok, head), F32)
    for i in range(row):
        for k in range(wide // head):
            v = own[i, :, k * head:(k + 1) * head].astype(F32)
            total = total + v * v
    inv = lax.rsqrt(jnp.sum(total, axis=-1, keepdims=True) / model + NORM_EPS)
    logits = jnp.zeros((n_tok, experts), F32)
    for i in range(row):
        for k in range(wide // head):
            d = i * (wide // head) + k
            v = own[i, :, k * head:(k + 1) * head].astype(F32)
            g = (v * inv * packs[d // row, d % row, 2:3, :]).astype(BF16)
            w = packs[d // row, d % row, 8:8 + experts, :].astype(BF16)
            logits = logits + dot_nt(g, w)
    logit_out[...] = logits + br_ref[...]
    for copy in outs:
        copy.wait()
    landed(res.at[0], s_res.at[0])
    sends.finish()


def dma(*shape):
    return pltpu.SemaphoreType.DMA(shape)


def solution(mesh):
    row_spec = P(('dp', 'fsdp'))
    shard_spec = P('fsdp')
    whole_spec = P()
    n_dev = mesh.shape[AXIS]
    side = math.isqrt(n_dev // CORES)
    row = side * CORES
    hbm = pl.BlockSpec(memory_space=pl.ANY)
    vmem = pl.BlockSpec(memory_space=pltpu.VMEM)
    smem = pl.BlockSpec(memory_space=pltpu.SMEM)

    def local_step(tokens, k_cache, v_cache, prefix_len, rope_cos, rope_sin, norm_attn, w_qkv, b_qkv, sink_logits, w_out, b_out, norm_router, w_router, b_router):
        n_req, n_new, model = tokens.shape
        kv, head = k_cache.shape[2:]
        heads = sink_logits.shape[0]
        experts = b_router.shape[0]
        depth = w_qkv.shape[0]
        n_tok = n_req * n_new
        wide = w_qkv.shape[1] // row
        ow = model // row
        flat = tokens.reshape(n_tok, model)
        cs = jnp.concatenate([rope_cos, rope_sin], axis=-1).reshape(n_tok, head)
        core = lax.rem(lax.axis_index(AXIS), CORES)
        bias_pad = lax.dynamic_update_slice(jnp.zeros((3 * head,), F32), b_qkv.astype(F32), (core * b_qkv.shape[0],))
        pack = jnp.concatenate([
            norm_attn.astype(F32)[None], b_out.astype(F32)[None], norm_router.astype(F32)[None],
            bias_pad.reshape(3, head), jnp.zeros((2, head), F32), w_router.astype(F32).T], axis=0)
        n_pack = pack.shape[0]

        qkv, xb, packs, wo = pl.pallas_call(
            functools.partial(project_kernel, side, heads, kv),
            out_shape=(jax.ShapeDtypeStruct((row, n_tok, wide), BF16),
                       jax.ShapeDtypeStruct((row, n_tok, ow), BF16),
                       jax.ShapeDtypeStruct((side, row, n_pack, head), F32),
                       jax.ShapeDtypeStruct((row, depth, ow), BF16)),
            in_specs=[hbm, hbm, hbm, vmem, vmem],
            out_specs=(hbm, hbm, hbm, hbm),
            scratch_shapes=[
                pltpu.VMEM((row - 1, depth, wide), BF16),
                pltpu.VMEM((row, depth, ow), BF16),
                pltpu.VMEM((side, row, depth, wide), BF16),
                pltpu.VMEM((row, n_tok, model), BF16),
                pltpu.VMEM((row, n_tok, model), BF16),
                pltpu.VMEM((row, n_tok, head), F32),
                pltpu.VMEM((side, row, n_pack, head), F32),
                pltpu.VMEM((side, CORES * n_tok, wide), F32),
                pltpu.VMEM((row, n_tok, wide), BF16),
                pltpu.VMEM((row, n_tok, ow), BF16),
                dma(row), dma(row), dma(4), dma(row), dma(row), dma(row), dma(row), dma(row), dma(row),
                dma(row), dma(row), dma(3), dma(3), dma(6), dma(6), dma(row), dma(row),
                dma(row), dma(row), dma(row), dma(row), dma(row), dma(row), dma(row), dma(row)],
            compiler_params=pltpu.CompilerParams(collective_id=0, has_side_effects=True, vmem_limit_bytes=60 * 2**20),
            name='project',
        )(w_qkv, w_out, flat, cs, pack)

        block = 512
        o = pl.pallas_call(
            functools.partial(attend_kernel, kv),
            out_shape=jax.ShapeDtypeStruct((n_tok, model), BF16),
            in_specs=[smem, smem, vmem, hbm, hbm],
            out_specs=vmem,
            scratch_shapes=[
                pltpu.VMEM((2, block, kv, head), BF16), pltpu.VMEM((2, block, kv, head), BF16),
                pltpu.VMEM((kv, block, head), BF16), pltpu.VMEM((kv, block, head), BF16),
                pltpu.VMEM((kv, heads // kv * n_new, head), F32), pltpu.VMEM((kv, heads // kv * n_new, head), F32),
                pltpu.VMEM((kv, heads // kv * n_new, head), F32), dma(2), dma(2)],
            compiler_params=pltpu.CompilerParams(vmem_limit_bytes=48 * 2**20),
            name='attend',
        )(prefix_len, sink_logits, qkv, k_cache, v_cache)

        resid, logits = pl.pallas_call(
            functools.partial(output_kernel, side, experts),
            out_shape=(jax.ShapeDtypeStruct((n_tok, model), BF16), jax.ShapeDtypeStruct((n_tok, experts), F32)),
            in_specs=[hbm, hbm, hbm, vmem, vmem],
            out_specs=(hbm, vmem),
            scratch_shapes=[
                pltpu.VMEM((row, n_tok, model), BF16),
                pltpu.VMEM((side, row, depth, ow), BF16),
                pltpu.VMEM((row, n_tok, ow), BF16),
                pltpu.VMEM((side, CORES * n_tok, ow), F32),
                pltpu.VMEM((row, n_tok, ow), BF16),
                pltpu.VMEM((row, n_tok, ow), BF16),
                dma(3 + row), dma(6), dma(6), dma(row), dma(row),
                dma(row), dma(row), dma(row), dma(row), dma(row), dma(row), dma(row), dma(row)],
            compiler_params=pltpu.CompilerParams(collective_id=1, has_side_effects=True, vmem_limit_bytes=48 * 2**20),
            name='output',
        )(o, wo, xb, packs, b_router.reshape(1, experts))

        split = qkv.reshape(row, n_req, n_new, wide)
        gw = wide - 2 * head
        k_new = jnp.transpose(split[..., gw:gw + head], (1, 2, 0, 3))
        v_new = jnp.transpose(split[..., gw + head:], (1, 2, 0, 3))
        return (resid.reshape(n_req, n_new, model), logits.reshape(n_req, n_new, experts), k_new, v_new)

    in_specs = (row_spec, row_spec, row_spec, row_spec, row_spec, row_spec, shard_spec, shard_spec, shard_spec, whole_spec, shard_spec, shard_spec, shard_spec, shard_spec, whole_spec)
    out_specs = (row_spec, row_spec, row_spec, row_spec)
    return jax.shard_map(local_step, mesh=mesh, in_specs=in_specs, out_specs=out_specs, check_vma=False)
```

```python
import functools
import math

import jax
import jax.numpy as jnp
from jax import lax
from jax.experimental import pallas as pl
from jax.experimental.pallas import tpu as pltpu
from jax.sharding import PartitionSpec as P

NORM_EPS = 1e-5
AXIS = 'fsdp'
CORES = 2
MESH_ID = pl.DeviceIdType.MESH
BF16 = jnp.bfloat16
F32 = jnp.float32
LOG2E = 1.4426950408889634


class Place:
    def __init__(self, side, across=False):
        index = lax.axis_index(AXIS)
        self.side, self.across = side, across
        self.row = side * CORES
        self.c = lax.rem(index, CORES)
        x = lax.rem(index // CORES, side)
        y = index // self.row
        self.a, self.b = (y, x) if across else (x, y)
        self.j = self.a * CORES + self.c

    def device(self, a, b, c):
        return (a * self.side + b) * CORES + c if self.across else (b * self.side + a) * CORES + c

    def spot(self, da, other=False):
        core = (1 - self.c) if other else self.c
        return lax.rem(self.a + da, self.side) * CORES + core

    def line(self, db):
        return lax.rem(self.b + db, self.side)

    def mate(self, da, other=False):
        return self.device(lax.rem(self.a + da, self.side), self.b, (1 - self.c) if other else self.c)

    def above(self, db):
        return self.device(self.a, self.line(db), self.c)

    def mates(self):
        return [self.mate(da, other) for da in range(self.side) for other in (False, True) if da or other]


class Sends:
    def __init__(self):
        self.started = []

    def __call__(self, src, dst, send_sem, recv_sem, device, later=None):
        pltpu.make_async_remote_copy(
            src_ref=src, dst_ref=dst, send_sem=send_sem, recv_sem=recv_sem,
            device_id={AXIS: device}, device_id_type=MESH_ID).start()
        self.started.append(later or (lambda: (src, send_sem)))

    def finish(self):
        for later in self.started:
            landed(*later())


def landed(ref, sem):
    pltpu.make_async_copy(ref, ref, sem).wait()


def meet(peers):
    barrier = pltpu.get_barrier_semaphore()
    for peer in peers:
        pl.semaphore_signal(barrier, inc=1, device_id={AXIS: peer}, device_id_type=MESH_ID)
    pl.semaphore_wait(barrier, len(peers))


def rel_order(side):
    return [(0, True), (1, False), (side - 1, False), (1, True), (side - 1, True), (2, False), (2, True)]


def mirror(rel, k, side):
    da, other = rel[k]
    return rel.index(((side - da) % side, other))


class RowGather:
    def __init__(self, place, sends, view, count, plus, minus, far, pair):
        self.p, self.sends, self.view, self.count = place, sends, view, count
        self.plus, self.minus, self.far_sems, self.pair_sems = plus, minus, far, pair

    def go(self, spot, k, sems, slot, da, other=False):
        v = self.view(spot, k)
        self.sends(v, v, sems[0].at[slot], sems[1].at[slot], self.p.mate(da, other), lambda: (self.view(0, k), sems[0].at[slot]))

    def own(self, k):
        p = self.p
        self.go(p.j, k, self.plus, k, 1)
        self.go(p.j, k, self.minus, k, p.side - 1)
        self.go(p.j, k, self.pair_sems, k, 0, True)

    def near(self, k):
        p, back, n = self.p, self.p.side - 1, self.count
        low, high = p.spot(back), p.spot(1)
        landed(self.view(low, k), self.plus[1].at[k])
        if k % 2 == 0:
            self.go(low, k, self.far_sems, k, 1)
        self.go(low, k, self.pair_sems, n + k, 0, True)
        landed(self.view(high, k), self.minus[1].at[k])
        if k % 2 == 1:
            self.go(high, k, self.far_sems, k, back)
        self.go(high, k, self.pair_sems, 2 * n + k, 0, True)

    def far(self, k):
        spot = self.p.spot(2)
        landed(self.view(spot, k), self.far_sems[1].at[k])
        self.go(spot, k, self.pair_sems, 3 * self.count + k, 0, True)

    def from_pair(self, da):
        group = {0: 0, self.p.side - 1: 1, 1: 2, 2: 3}[da]
        for k in range(self.count):
            landed(self.view(self.p.spot(da, True), k), self.pair_sems[1].at[group * self.count + k])


class ColumnGather:
    def __init__(self, place, sends, buf, up, down, far):
        self.p, self.sends, self.buf = place, sends, buf
        self.up, self.down, self.far_sems = up, down, far
        self.order = [(0, False)] + rel_order(place.side)

    def go(self, line, k, sems, db):
        v = self.buf.at[line, self.p.spot(*self.order[k])]
        self.sends(v, v, sems[0].at[k], sems[1].at[k], self.p.above(db), lambda: (self.buf.at[0, 0], sems[0].at[k]))

    def own(self, k):
        self.go(self.p.b, k, self.up, 1)
        self.go(self.p.b, k, self.down, self.p.side - 1)

    def near(self, k):
        p, back = self.p, self.p.side - 1
        spot = p.spot(*self.order[k])
        landed(self.buf.at[p.line(back), spot], self.up[1].at[k])
        if k % 2 == 0:
            self.go(p.line(back), k, self.far_sems, 1)
        landed(self.buf.at[p.line(1), spot], self.down[1].at[k])
        if k % 2 == 1:
            self.go(p.line(1), k, self.far_sems, back)

    def far(self, k):
        landed(self.buf.at[self.p.line(2), self.p.spot(*self.order[k])], self.far_sems[1].at[k])


def dot_nt(a, b):
    return lax.dot_general(a, b, (((1,), (1,)), ((), ())), preferred_element_type=F32)


def project_kernel(side, heads, kv, w_ref, wo_ref, x_ref, cs_ref, pack_ref, k_ref, v_ref,
                   qkv_out, xb_out, pack_out, wo_out, kt_out, vt_out,
                   wl, wol, wq, xa, hh, csa, packs, acc, res, kin, vin, kmid, vmid,
                   s_wl, s_wol, s_loc, s_a2a, r_a2a, s_o, r_o, s_x, r_x, s_cs, r_cs, s_pk, r_pk, s_pv, r_pv,
                   s_plus, r_plus, s_minus, r_minus, s_rfar, r_rfar, s_pair, r_pair,
                   s_up, r_up, s_dn, r_dn, s_far, r_far, s_res, r_res, s_in, s_mid):
    p = Place(side)
    t = Place(side, across=True)
    row = p.row
    back = side - 1
    head = w_ref.shape[1] // (heads + 2 * kv)
    qw = heads // kv * head
    depth = w_ref.shape[0]
    wide = qw + 2 * head
    ow = wol.shape[-1]
    rel = rel_order(side)
    sends = Sends()

    def take(spot, dst, sem):
        parts = ((spot * qw, qw, 0), (heads * head + spot * head, head, qw),
                 ((heads + kv) * head + spot * head, head, qw + head))
        for start, size, at in parts:
            pltpu.make_async_copy(w_ref.at[:, pl.ds(pl.multiple_of(start, head), size)],
                                  dst.at[:, pl.ds(at, size)], sem).start()

    take(p.j, wq.at[p.b, p.j], s_wl.at[0])
    for k, at in enumerate(rel):
        take(p.spot(*at), wl.at[k], s_wl.at[k + 1])
    pltpu.make_async_copy(x_ref, xa.at[p.j], s_loc.at[0]).start()
    for k, at in enumerate(rel + [(0, False)]):
        pltpu.make_async_copy(wo_ref.at[:, pl.ds(pl.multiple_of(t.spot(*at) * ow, head), ow)], wol.at[k],
                              s_wol.at[k]).start()

    depth_in, block = kin.shape[0], kin.shape[1]
    per = k_ref.shape[1] // block
    steps = k_ref.shape[0] * per

    def bring(b, slot):
        r, at = b // per, lax.rem(b, per) * block
        return (pltpu.make_async_copy(k_ref.at[r, pl.ds(at, block)], kin.at[slot], s_in.at[slot]),
                pltpu.make_async_copy(v_ref.at[r, pl.ds(at, block)], vin.at[slot], s_in.at[depth_in + slot]))

    def put(b, slot):
        r, at = b // per, lax.rem(b, per) * block
        return (pltpu.make_async_copy(kmid.at[slot], kt_out.at[r, :, pl.ds(at, block)], s_mid.at[slot]),
                pltpu.make_async_copy(vmid.at[slot], vt_out.at[r, :, pl.ds(at, block)], s_mid.at[depth_in + slot]))

    def turn(b, _):
        slot = lax.rem(b, depth_in)
        for copy in bring(b, slot):
            copy.wait()

        @pl.when(b >= depth_in)
        def _():
            for copy in put(b - depth_in, slot):
                copy.wait()
        kmid[slot] = pltpu.einshape('skd->ksd', kin[slot])
        vmid[slot] = pltpu.einshape('skd->ksd', vin[slot])
        for copy in put(b, slot):
            copy.start()

        @pl.when(b + depth_in < steps)
        def _():
            for copy in bring(b + depth_in, slot):
                copy.start()
        return 0

    done = [0]

    def fill(n):
        n = min(n, steps - done[0])
        if n > 0:
            lax.fori_loop(done[0], done[0] + n, turn, 0)
            done[0] += n

    for b in range(depth_in):
        for copy in bring(b, b):
            copy.start()
    packs[p.b, p.j] = pack_ref[...]
    csa[p.j] = cs_ref[...]

    meet(p.mates() + [t.mate(da, other) for da in range(1, side) for other in (False, True)])

    gather = ColumnGather(p, sends, wq, (s_up, r_up), (s_dn, r_dn), (s_far, r_far))
    count = r_plus.shape[0]
    cut = xa.shape[1] // count
    tokens = RowGather(p, sends, lambda spot, k: xa.at[spot, pl.ds(k * cut, cut)], count,
                       (s_plus, r_plus), (s_minus, r_minus), (s_rfar, r_rfar), (s_pair, r_pair))
    landed(wq.at[p.b, p.j], s_wl.at[0])
    gather.own(0)
    for k, at in enumerate(rel):
        sends(pack_ref, packs.at[p.b, p.j], s_pk.at[k], r_pk.at[k], p.mate(*at))
    for k, at in enumerate(rel):
        landed(wl.at[k], s_wl.at[k + 1])
        sends(wl.at[k], wq.at[p.b, p.j], s_a2a.at[k], r_a2a.at[k], p.mate(*at))
    for k, at in enumerate(rel):
        sends(cs_ref, csa.at[p.j], s_cs.at[k], r_cs.at[k], p.mate(*at))
    landed(xa.at[p.j], s_loc.at[0])
    for k in range(count):
        tokens.own(k)

    for k in range(row - 1):
        landed(packs.at[p.b, p.spot(*rel[k])], r_pk.at[mirror(rel, k, side)])
    pv = packs.at[p.b]
    sends(pv, pv, s_pv.at[0], r_pv.at[0], p.above(1))
    sends(pv, pv, s_pv.at[1], r_pv.at[1], p.above(back))
    for k in range(row - 1):
        landed(wq.at[p.b, p.spot(*rel[k])], r_a2a.at[mirror(rel, k, side)])
        gather.own(k + 1)
        fill(2)
    pu = packs.at[p.line(back)]
    landed(pu, r_pv.at[0])
    sends(pu, pu, s_pv.at[2], r_pv.at[2], p.above(1))
    landed(packs.at[p.line(1)], r_pv.at[1])
    landed(packs.at[p.line(2)], r_pv.at[2])
    for k in range(row - 1):
        landed(csa.at[p.spot(*rel[k])], r_cs.at[mirror(rel, k, side)])
    out_pack = pltpu.make_async_copy(packs, pack_out, s_loc.at[2])
    out_pack.start()

    model = xa.shape[-1]

    def norm(spot):
        total = jnp.zeros((xa.shape[1], head), F32)
        for i in range(model // head):
            v = xa[spot, :, i * head:(i + 1) * head].astype(F32)
            total = total + v * v
        inv = lax.rsqrt(jnp.sum(total, axis=-1, keepdims=True) / model + NORM_EPS)
        for i in range(model // head):
            v = xa[spot, :, i * head:(i + 1) * head].astype(F32)
            g = packs[i // row, i % row, 0:1, :]
            hh[spot, :, i * head:(i + 1) * head] = (v * inv * g).astype(BF16)

    span = row * depth

    def part(da, db):
        chip = lax.rem(p.a + da, side)
        rows = hh[pl.ds(chip * CORES, CORES), :, pl.ds(pl.multiple_of(p.line(db) * span, span), span)]
        rows = rows.reshape(CORES * hh.shape[1], span)
        return jnp.dot(rows, wq[p.line(db)].reshape(span, wide), preferred_element_type=F32)

    def bias(m):
        e, k = m // 3, lax.rem(m, 3)
        out = 0.0
        for c in range(CORES):
            d = e * CORES + c
            out = out + packs[d // row, lax.rem(d, row), pl.ds(3 + k, 1), :]
        return out

    lanes = lax.broadcasted_iota(jnp.int32, (1, head), 1)

    def finish(da):
        total = acc[da] + part(da, 2)
        chip = lax.rem(p.a + da, side)
        cs = csa[pl.ds(chip * CORES, CORES)].reshape(CORES * csa.shape[1], head)
        turned = pltpu.roll(cs, head // 2, 1)
        low = lanes < head // 2
        cos = jnp.where(low, cs, turned)
        sin = jnp.where(low, -turned, cs)
        n_q = heads // kv
        for i in range(n_q + 2):
            m = p.j * n_q + i if i < n_q else (heads + p.j if i == n_q else heads + kv + p.j)
            v = total[:, i * head:(i + 1) * head] + bias(m)
            if i <= n_q:
                v = v * cos + pltpu.roll(v, head // 2, 1) * sin
            res[da * CORES:(da + 1) * CORES, :, i * head:(i + 1) * head] = v.astype(BF16).reshape(CORES, -1, head)
        for c in range(CORES):
            src = res.at[da * CORES + c]
            if da:
                sends(src, qkv_out.at[p.j], s_res.at[da * CORES + c], r_res.at[p.j], p.device(chip, p.b, c))
            else:
                @pl.when(p.c == c)
                def _():
                    pltpu.make_async_copy(src, qkv_out.at[p.j], r_res.at[p.j]).start()

                @pl.when(p.c != c)
                def _():
                    pltpu.make_async_remote_copy(
                        src_ref=src, dst_ref=qkv_out.at[p.j], send_sem=s_res.at[0], recv_sem=r_res.at[p.j],
                        device_id={AXIS: p.device(chip, p.b, c)}, device_id_type=MESH_ID).start()

    norm(p.spot(0))
    tokens.from_pair(0)
    norm(p.spot(0, True))
    for k in range(0, 4):
        gather.near(k)
        fill(2)
    acc[0] = part(0, 0)
    for k in range(count):
        if k % 2 == 0:
            for i in range(4 + k, 4 + k + 2):
                gather.near(i)
            fill(2)
        tokens.near(k)
        fill(2)
    for k, at in enumerate(rel):
        landed(wol.at[k], s_wol.at[k])
        sends(wol.at[k], wo_out.at[t.j], s_o.at[k], r_o.at[k], t.mate(*at))
    for k, at in enumerate(rel):
        src = xa.at[p.j, :, pl.ds(pl.multiple_of(t.spot(*at) * ow, head), ow)]
        sends(src, xb_out.at[t.j], s_x.at[k], r_x.at[k], t.mate(*at))
    landed(wol.at[row - 1], s_wol.at[row - 1])
    own_o = pltpu.make_async_copy(wol.at[row - 1], wo_out.at[t.j], s_loc.at[1])
    own_o.start()
    own_x = pltpu.make_async_copy(xa.at[p.j, :, pl.ds(pl.multiple_of(t.j * ow, head), ow)], xb_out.at[t.j], s_loc.at[3])
    own_x.start()
    fill(steps)
    acc[0] += part(0, 1)
    acc[0] += part(0, back)
    for da in (back, 1):
        norm(p.spot(da))
        tokens.from_pair(da)
        norm(p.spot(da, True))
        acc[da] = part(da, 0)
        acc[da] += part(da, 1)
        acc[da] += part(da, back)
    for k in range(count):
        tokens.far(k)
    norm(p.spot(2))
    tokens.from_pair(2)
    norm(p.spot(2, True))
    for k in range(row):
        gather.far(k)
    finish(1)
    finish(back)
    acc[2] = part(2, 0)
    acc[2] += part(2, 1)
    acc[2] += part(2, back)
    finish(2)
    finish(0)
    for k in range(row - 1):
        landed(wo_out.at[t.spot(*rel[k])], r_o.at[mirror(rel, k, side)])
        landed(xb_out.at[t.spot(*rel[k])], r_x.at[mirror(rel, k, side)])
    for b in range(steps - depth_in, steps):
        for copy in put(b, b % depth_in):
            copy.wait()
    for i in range(row):
        landed(qkv_out.at[i], r_res.at[i])
    own_o.wait()
    own_x.wait()
    out_pack.wait()
    landed(res.at[0], s_res.at[0])
    sends.finish()


def output_kernel(side, kv, experts, len_ref, sink_ref, qkv_ref, kt_ref, vt_ref, wo_ref, xb_ref, packs, br_ref,
                  resid_out, logit_out,
                  kb0, kb1, vb0, vb1, sb0, sb1, mb0, mb1, lb0, lb1, oa, wq, xbv, acc, res, own,
                  s_k, s_v, s_loc, s_plus, r_plus, s_minus, r_minus, s_rfar, r_rfar, s_pair, r_pair,
                  s_up, r_up, s_dn, r_dn, s_far, r_far, s_res, r_res):
    p = Place(side, across=True)
    row = p.row
    back = side - 1
    head = packs.shape[-1]
    depth = wq.shape[2]
    wide = wq.shape[3]
    n_tok = oa.shape[1]
    n_req = kt_ref.shape[0]
    slots = kt_ref.shape[2]
    new = n_tok // n_req
    group = qkv_ref.shape[2] // head - 2
    rows = group * new
    total = n_req * kv
    scale = head ** -0.5 * LOG2E
    block = min(512, slots)
    sends = Sends()
    loads = [pltpu.make_async_copy(wo_ref, wq.at[p.b], s_loc.at[0]),
             pltpu.make_async_copy(xb_ref, xbv, s_loc.at[1])]
    for copy in loads:
        copy.start()

    def fetch(n, which, buf, sem):
        n = jnp.minimum(n, total - 1)
        return pltpu.make_async_copy(which.at[n // kv, lax.rem(n, kv)], buf, sem)

    fetch(0, kt_ref, kb0, s_k.at[0]).start()
    fetch(0, vt_ref, vb0, s_v.at[0]).start()
    fetch(1, kt_ref, kb1, s_k.at[1]).start()
    fetch(1, vt_ref, vb1, s_v.at[1]).start()
    meet(p.mates() + [p.above(1), p.above(back)])
    gather = ColumnGather(p, sends, wq, (s_up, r_up), (s_dn, r_dn), (s_far, r_far))
    lanes = row * wide // 2
    tokens = RowGather(
        p, sends, lambda spot, k: oa.at[spot, pl.ds(k // 2 * new, new), pl.ds(k % 2 * lanes, lanes)], 2 * n_req,
        (s_plus, r_plus), (s_minus, r_minus), (s_rfar, r_rfar), (s_pair, r_pair))
    count = tokens.count
    loads[0].wait()
    for k in range(row):
        gather.own(k)
    loads[1].wait()

    def place(r):
        return pl.ds(pl.multiple_of(r * new, new), new)

    ri = lax.rem(lax.broadcasted_iota(jnp.int32, (rows, head), 0), new)
    ci = lax.broadcasted_iota(jnp.int32, (rows, head), 1)

    def first(n, sb, mb, lb, kb):
        n = jnp.minimum(n, total - 1)
        r, i = n // kv, lax.rem(n, kv)
        q = jnp.concatenate([qkv_ref[i, place(r), g * head:(g + 1) * head] for g in range(group)], axis=0)
        length = len_ref[r]
        kn = qkv_ref[i, place(r), group * head:(group + 1) * head]
        kn = jnp.concatenate([kn, jnp.zeros((head - new, head), BF16)], axis=0)
        s = jnp.where(ri >= ci, dot_nt(q, kn), -1e30)
        sb[:, slots:] = s
        m = s
        for b in range(slots // block):
            s = dot_nt(q, kb[b * block:(b + 1) * block])
            s = jnp.where(b * block + lax.broadcasted_iota(jnp.int32, (1, block), 1) < length, s, -1e30)
            sb[:, b * block:(b + 1) * block] = s
            for k in range(block // head):
                m = jnp.maximum(m, s[:, k * head:(k + 1) * head])
            yield
        m = jnp.max(m, axis=-1, keepdims=True) * scale
        sink = jnp.concatenate([jnp.full((new, head), sink_ref[i * group + g] * LOG2E, F32) for g in range(group)], axis=0)
        m = jnp.maximum(m, sink)
        mb[...] = m
        lb[...] = jnp.exp2(sink - m)

    def second(n, sb, mb, lb, vb):
        r, i = n // kv, lax.rem(n, kv)
        m = mb[...]
        vn = qkv_ref[i, place(r), (group + 1) * head:]
        vn = jnp.concatenate([vn, jnp.zeros((head - new, head), BF16)], axis=0)
        pr = jnp.exp2(sb[:, slots:] * scale - m)
        low = pr
        out = jnp.dot(pr.astype(BF16), vn, preferred_element_type=F32)
        for b in range(slots // block):
            prs = []
            for k in range(block // head):
                at = b * block + k * head
                pr = jnp.exp2(sb[:, at:at + head] * scale - m)
                low = low + pr
                prs.append(pr.astype(BF16))
            out = out + jnp.dot(jnp.concatenate(prs, axis=1), vb[b * block:(b + 1) * block], preferred_element_type=F32)
            yield
        out = (out / (jnp.sum(low, axis=-1, keepdims=True) + lb[...])).astype(BF16)
        for g in range(group):
            at = pl.multiple_of((i * group + g) * head, head)
            oa[p.j, place(r), pl.ds(at, head)] = out[g * new:(g + 1) * new]

    def run(*work):
        work = list(work)
        while work:
            for w in list(work):
                if next(w, w) is w:
                    work.remove(w)

    fetch(0, kt_ref, kb0, s_k.at[0]).wait()
    run(first(0, sb0, mb0, lb0, kb0))
    fetch(2, kt_ref, kb0, s_k.at[0]).start()
    turns = total // 2
    each = turns // count

    def events(h):
        out = []
        if (h + 1) % each == 0:
            out.append((tokens.own, h // each))
        for k in range(count):
            if h == (k + 2) * each:
                out.append((tokens.near, k))
            if h == (k + 3) * each + each // 2:
                out.append((tokens.far, k))
        if h >= turns // 2:
            for k in range(row):
                if turns // 2 + k // 2 == h:
                    out.append((gather.near, k))
        return out

    def body(h, _):
        n = 2 * h
        fetch(n, vt_ref, vb0, s_v.at[0]).wait()
        fetch(n + 1, kt_ref, kb1, s_k.at[1]).wait()
        run(first(n + 1, sb1, mb1, lb1, kb1), second(n, sb0, mb0, lb0, vb0))
        fetch(n + 2, vt_ref, vb0, s_v.at[0]).start()
        fetch(n + 3, kt_ref, kb1, s_k.at[1]).start()
        fetch(n + 1, vt_ref, vb1, s_v.at[1]).wait()
        fetch(n + 2, kt_ref, kb0, s_k.at[0]).wait()
        run(first(n + 2, sb0, mb0, lb0, kb0), second(n + 1, sb1, mb1, lb1, vb1))
        fetch(n + 3, vt_ref, vb1, s_v.at[1]).start()
        fetch(n + 4, kt_ref, kb0, s_k.at[0]).start()
        for at in range(turns):
            todo = events(at)
            if todo:
                @pl.when(h == at)
                def _():
                    for act, k in todo:
                        act(k)
        return 0

    lax.fori_loop(0, turns, body, 0)
    for which, buf, sem in ((vt_ref, vb0, s_v.at[0]), (vt_ref, vb1, s_v.at[1]), (kt_ref, kb0, s_k.at[0]), (kt_ref, kb1, s_k.at[1])):
        fetch(0, which, buf, sem).wait()
    past = [e for h in range(turns) for e in events(h)]

    def rest(act, k):
        if not any(a == act and i == k for a, i in past):
            act(k)

    def part(da, db):
        chip = lax.rem(p.a + da, side)
        cols = [oa[pl.ds(chip * CORES, CORES), :, pl.ds(pl.multiple_of(p.device(a, p.line(db), 0) * depth, depth), CORES * depth)]
                for a in range(side)]
        lhs = jnp.concatenate([v.reshape(CORES * n_tok, CORES * depth) for v in cols], axis=-1)
        return jnp.dot(lhs, wq[p.line(db)].reshape(row * depth, wide), preferred_element_type=F32)

    def finish(da):
        total = acc[da] + part(da, 2)
        chip = lax.rem(p.a + da, side)
        for i in range(wide // head):
            d = p.j * (wide // head) + i
            b = packs[d // row, lax.rem(d, row), 1:2, :]
            at = pl.ds(i * head, head)
            base = xbv[pl.ds(chip * CORES, CORES), :, at].reshape(-1, head).astype(F32)
            v = base + (total[:, i * head:(i + 1) * head] + b)
            res[da * CORES:(da + 1) * CORES, :, at] = v.astype(BF16).reshape(CORES, -1, head)
        for c in range(CORES):
            src = res.at[da * CORES + c]
            if da:
                sends(src, own.at[p.j], s_res.at[da * CORES + c], r_res.at[p.j], p.device(chip, p.b, c))
            else:
                @pl.when(p.c == c)
                def _():
                    own[p.j] = src[...]

                @pl.when(p.c != c)
                def _():
                    pltpu.make_async_remote_copy(
                        src_ref=src, dst_ref=own.at[p.j], send_sem=s_res.at[0], recv_sem=r_res.at[p.j],
                        device_id={AXIS: p.device(chip, p.b, c)}, device_id_type=MESH_ID).start()

    for k in range(row):
        rest(gather.near, k)
    for k in range(count):
        rest(tokens.near, k)
        if k:
            rest(tokens.far, k - 1)
    tokens.from_pair(0)
    acc[0] = part(0, 0)
    acc[0] += part(0, 1)
    acc[0] += part(0, back)
    for da in (back, 1):
        tokens.from_pair(da)
        acc[da] = part(da, 0)
        acc[da] += part(da, 1)
        acc[da] += part(da, back)
    rest(tokens.far, count - 1)
    for k in range(row):
        gather.far(k)
    finish(1)
    finish(back)
    tokens.from_pair(2)
    acc[2] = part(2, 0)
    acc[2] += part(2, 1)
    acc[2] += part(2, back)
    finish(2)
    finish(0)
    for da, other in rel_order(side):
        spot = p.spot(da, other)
        landed(own.at[spot], r_res.at[spot])
    model = row * wide
    outs = []
    for i in range(row):
        copy = pltpu.make_async_copy(own.at[i], resid_out.at[:, pl.ds(i * wide, wide)], s_loc.at[3 + i])
        copy.start()
        outs.append(copy)
    square = jnp.zeros((n_tok, head), F32)
    for i in range(row):
        for k in range(wide // head):
            v = own[i, :, k * head:(k + 1) * head].astype(F32)
            square = square + v * v
    inv = lax.rsqrt(jnp.sum(square, axis=-1, keepdims=True) / model + NORM_EPS)
    logits = jnp.zeros((n_tok, experts), F32)
    for i in range(row):
        for k in range(wide // head):
            d = i * (wide // head) + k
            v = own[i, :, k * head:(k + 1) * head].astype(F32)
            g = (v * inv * packs[d // row, d % row, 2:3, :]).astype(BF16)
            w = packs[d // row, d % row, 8:8 + experts, :].astype(BF16)
            logits = logits + dot_nt(g, w)
    logit_out[...] = logits + br_ref[...]
    for copy in outs:
        copy.wait()
    landed(res.at[0], s_res.at[0])
    sends.finish()


def dma(*shape):
    return pltpu.SemaphoreType.DMA(shape)


def solution(mesh):
    row_spec = P(('dp', 'fsdp'))
    shard_spec = P('fsdp')
    whole_spec = P()
    n_dev = mesh.shape[AXIS]
    side = math.isqrt(n_dev // CORES)
    row = side * CORES
    hbm = pl.BlockSpec(memory_space=pl.ANY)
    vmem = pl.BlockSpec(memory_space=pltpu.VMEM)
    smem = pl.BlockSpec(memory_space=pltpu.SMEM)

    def local_step(tokens, k_cache, v_cache, prefix_len, rope_cos, rope_sin, norm_attn, w_qkv, b_qkv, sink_logits, w_out, b_out, norm_router, w_router, b_router):
        n_req, n_new, model = tokens.shape
        kv, head = k_cache.shape[2:]
        heads = sink_logits.shape[0]
        experts = b_router.shape[0]
        depth = w_qkv.shape[0]
        n_tok = n_req * n_new
        wide = w_qkv.shape[1] // row
        ow = model // row
        flat = tokens.reshape(n_tok, model)
        cs = jnp.concatenate([rope_cos, rope_sin], axis=-1).reshape(n_tok, head)
        core = lax.rem(lax.axis_index(AXIS), CORES)
        bias_pad = lax.dynamic_update_slice(jnp.zeros((3 * head,), F32), b_qkv.astype(F32), (core * b_qkv.shape[0],))
        pack = jnp.concatenate([
            norm_attn.astype(F32)[None], b_out.astype(F32)[None], norm_router.astype(F32)[None],
            bias_pad.reshape(3, head), jnp.zeros((2, head), F32), w_router.astype(F32).T], axis=0)
        n_pack = pack.shape[0]

        pieces = 4
        turn = 256
        slots = k_cache.shape[1]
        qkv, xb, packs, wo, kt, vt = pl.pallas_call(
            functools.partial(project_kernel, side, heads, kv),
            out_shape=(jax.ShapeDtypeStruct((row, n_tok, wide), BF16),
                       jax.ShapeDtypeStruct((row, n_tok, ow), BF16),
                       jax.ShapeDtypeStruct((side, row, n_pack, head), F32),
                       jax.ShapeDtypeStruct((row, depth, ow), BF16),
                       jax.ShapeDtypeStruct((n_req, kv, slots, head), BF16),
                       jax.ShapeDtypeStruct((n_req, kv, slots, head), BF16)),
            in_specs=[hbm, hbm, hbm, vmem, vmem, hbm, hbm],
            out_specs=(hbm,) * 6,
            scratch_shapes=[
                pltpu.VMEM((row - 1, depth, wide), BF16),
                pltpu.VMEM((row, depth, ow), BF16),
                pltpu.VMEM((side, row, depth, wide), BF16),
                pltpu.VMEM((row, n_tok, model), BF16),
                pltpu.VMEM((row, n_tok, model), BF16),
                pltpu.VMEM((row, n_tok, head), F32),
                pltpu.VMEM((side, row, n_pack, head), F32),
                pltpu.VMEM((side, CORES * n_tok, wide), F32),
                pltpu.VMEM((row, n_tok, wide), BF16),
                pltpu.VMEM((4, turn, kv, head), BF16), pltpu.VMEM((4, turn, kv, head), BF16),
                pltpu.VMEM((4, kv, turn, head), BF16), pltpu.VMEM((4, kv, turn, head), BF16),
                dma(row), dma(row), dma(4), dma(row), dma(row), dma(row), dma(row), dma(row), dma(row),
                dma(row), dma(row), dma(row), dma(row), dma(3), dma(3),
                dma(pieces), dma(pieces), dma(pieces), dma(pieces), dma(pieces), dma(pieces), dma(4 * pieces), dma(4 * pieces),
                dma(row), dma(row), dma(row), dma(row), dma(row), dma(row), dma(row), dma(row), dma(8), dma(8)],
            compiler_params=pltpu.CompilerParams(collective_id=0, has_side_effects=True, vmem_limit_bytes=60 * 2**20),
            name='project',
        )(w_qkv, w_out, flat, cs, pack, k_cache, v_cache)

        n_row = heads // kv * n_new
        resid, logits = pl.pallas_call(
            functools.partial(output_kernel, side, kv, experts),
            out_shape=(jax.ShapeDtypeStruct((n_tok, model), BF16), jax.ShapeDtypeStruct((n_tok, experts), F32)),
            in_specs=[smem, smem, vmem, hbm, hbm, hbm, hbm, vmem, vmem],
            out_specs=(hbm, vmem),
            scratch_shapes=[
                pltpu.VMEM((slots, head), BF16), pltpu.VMEM((slots, head), BF16),
                pltpu.VMEM((slots, head), BF16), pltpu.VMEM((slots, head), BF16),
                pltpu.VMEM((n_row, slots + head), F32), pltpu.VMEM((n_row, slots + head), F32),
                pltpu.VMEM((n_row, head), F32), pltpu.VMEM((n_row, head), F32),
                pltpu.VMEM((n_row, head), F32), pltpu.VMEM((n_row, head), F32),
                pltpu.VMEM((row, n_tok, model), BF16),
                pltpu.VMEM((side, row, depth, ow), BF16),
                pltpu.VMEM((row, n_tok, ow), BF16),
                pltpu.VMEM((side, CORES * n_tok, ow), F32),
                pltpu.VMEM((row, n_tok, ow), BF16),
                pltpu.VMEM((row, n_tok, ow), BF16),
                dma(2), dma(2), dma(3 + row),
                dma(pieces), dma(pieces), dma(pieces), dma(pieces), dma(pieces), dma(pieces), dma(4 * pieces), dma(4 * pieces),
                dma(row), dma(row), dma(row), dma(row), dma(row), dma(row), dma(row), dma(row)],
            compiler_params=pltpu.CompilerParams(collective_id=1, has_side_effects=True, vmem_limit_bytes=56 * 2**20),
            name='output',
        )(prefix_len, sink_logits, qkv, kt, vt, wo, xb, packs, b_router.reshape(1, experts))

        split = qkv.reshape(row, n_req, n_new, wide)
        gw = wide - 2 * head
        k_new = jnp.transpose(split[..., gw:gw + head], (1, 2, 0, 3))
        v_new = jnp.transpose(split[..., gw + head:], (1, 2, 0, 3))
        return (resid.reshape(n_req, n_new, model), logits.reshape(n_req, n_new, experts), k_new, v_new)

    in_specs = (row_spec, row_spec, row_spec, row_spec, row_spec, row_spec, shard_spec, shard_spec, shard_spec, whole_spec, shard_spec, shard_spec, shard_spec, shard_spec, whole_spec)
    out_specs = (row_spec, row_spec, row_spec, row_spec)
    return jax.shard_map(local_step, mesh=mesh, in_specs=in_specs, out_specs=out_specs, check_vma=False)
```

```python
import functools
import math

import jax
import jax.numpy as jnp
from jax import lax
from jax.experimental import pallas as pl
from jax.experimental.pallas import tpu as pltpu
from jax.sharding import PartitionSpec as P

NORM_EPS = 1e-5
AXIS = 'fsdp'
CORES = 2
MESH_ID = pl.DeviceIdType.MESH
BF16 = jnp.bfloat16
F32 = jnp.float32
LOG2E = 1.4426950408889634
SAME, OTHER = False, True
BOTH = (SAME, OTHER)


class Place:
    def __init__(self, side, across=False):
        index = lax.axis_index(AXIS)
        self.side, self.across = side, across
        self.row = side * CORES
        self.c = lax.rem(index, CORES)
        x = lax.rem(index // CORES, side)
        y = index // self.row
        self.a, self.b = (y, x) if across else (x, y)
        self.j = self.a * CORES + self.c

    def device(self, a, b, c):
        return (a * self.side + b) * CORES + c if self.across else (b * self.side + a) * CORES + c

    def spot(self, da, other=False):
        core = (1 - self.c) if other else self.c
        return lax.rem(self.a + da, self.side) * CORES + core

    def line(self, db):
        return lax.rem(self.b + db, self.side)

    def mate(self, da, other=False):
        return self.device(lax.rem(self.a + da, self.side), self.b, (1 - self.c) if other else self.c)

    def above(self, db):
        return self.device(self.a, self.line(db), self.c)

    def mates(self):
        return [self.mate(da, other) for da in range(self.side) for other in BOTH if da or other]


class Sends:
    def __init__(self):
        self.started = []

    def __call__(self, src, dst, send_sem, recv_sem, device, later=None):
        pltpu.make_async_remote_copy(
            src_ref=src, dst_ref=dst, send_sem=send_sem, recv_sem=recv_sem,
            device_id={AXIS: device}, device_id_type=MESH_ID).start()
        self.started.append(later or (lambda: (src, send_sem)))

    def finish(self):
        for later in self.started:
            landed(*later())


def landed(ref, sem):
    pltpu.make_async_copy(ref, ref, sem).wait()


def meet(peers):
    barrier = pltpu.get_barrier_semaphore()
    for peer in peers:
        pl.semaphore_signal(barrier, inc=1, device_id={AXIS: peer}, device_id_type=MESH_ID)
    pl.semaphore_wait(barrier, len(peers))


def rel_order(side):
    return [(0, OTHER), (1, SAME), (side - 1, SAME), (1, OTHER), (side - 1, OTHER), (2, SAME), (2, OTHER)]


def send_order(side):
    return [(0, OTHER), (1, SAME), (side - 1, SAME), (2, SAME), (2, OTHER), (1, OTHER), (side - 1, OTHER)]


class RowGather:
    def __init__(self, place, sends, view, count, plus, minus, far, pair):
        self.p, self.sends, self.view, self.count = place, sends, view, count
        self.plus, self.minus, self.far_sems, self.pair_sems = plus, minus, far, pair

    def go(self, spot, k, sems, slot, da, other=False):
        v = self.view(spot, k)
        self.sends(v, v, sems[0].at[slot], sems[1].at[slot], self.p.mate(da, other), lambda: (self.view(0, k), sems[0].at[slot]))

    def own(self, k):
        p = self.p
        self.go(p.j, k, self.plus, k, 1)
        self.go(p.j, k, self.minus, k, p.side - 1)
        self.go(p.j, k, self.pair_sems, k, 0, True)

    def near(self, k):
        p, back, n = self.p, self.p.side - 1, self.count
        low, high = p.spot(back), p.spot(1)
        landed(self.view(low, k), self.plus[1].at[k])
        if k % 2 == 0:
            self.go(low, k, self.far_sems, k, 1)
        self.go(low, k, self.pair_sems, n + k, 0, True)
        landed(self.view(high, k), self.minus[1].at[k])
        if k % 2 == 1:
            self.go(high, k, self.far_sems, k, back)
        self.go(high, k, self.pair_sems, 2 * n + k, 0, True)

    def far(self, k):
        spot = self.p.spot(2)
        landed(self.view(spot, k), self.far_sems[1].at[k])
        self.go(spot, k, self.pair_sems, 3 * self.count + k, 0, True)

    def from_pair(self, da):
        group = {0: 0, self.p.side - 1: 1, 1: 2, 2: 3}[da]
        for k in range(self.count):
            landed(self.view(self.p.spot(da, OTHER), k), self.pair_sems[1].at[group * self.count + k])


class ColumnGather:
    def __init__(self, place, sends, buf, up, down, far):
        self.p, self.sends, self.buf = place, sends, buf
        self.up, self.down, self.far_sems = up, down, far
        self.order = [(0, SAME)] + rel_order(place.side)

    def go(self, line, k, sems, db):
        v = self.buf.at[line, self.p.spot(*self.order[k])]
        self.sends(v, v, sems[0].at[k], sems[1].at[k], self.p.above(db), lambda: (self.buf.at[0, 0], sems[0].at[k]))

    def own(self, k):
        self.go(self.p.b, k, self.up, 1)
        self.go(self.p.b, k, self.down, self.p.side - 1)

    def near(self, k):
        p, back = self.p, self.p.side - 1
        spot = p.spot(*self.order[k])
        landed(self.buf.at[p.line(back), spot], self.up[1].at[k])
        if k % 2 == 0:
            self.go(p.line(back), k, self.far_sems, 1)
        landed(self.buf.at[p.line(1), spot], self.down[1].at[k])
        if k % 2 == 1:
            self.go(p.line(1), k, self.far_sems, back)

    def far(self, k):
        landed(self.buf.at[self.p.line(2), self.p.spot(*self.order[k])], self.far_sems[1].at[k])


class Exchange:
    def __init__(self, place, sends, src, dst, relay, sems, hand_sems):
        self.p, self.sends, self.src, self.dst, self.relay = place, sends, src, dst, relay
        (self.s, self.r), (self.hs, self.hr, self.fs) = sems, hand_sems

    def send(self, da, other):
        p, slot = self.p, da * CORES + other
        if da == 2:
            way = p.side - 1 if other else 1
            self.sends(self.src(da, other), self.relay.at[int(other)], self.hs.at[int(other)], self.hr.at[int(other)],
                       p.mate(way))
        else:
            self.sends(self.src(da, other), self.dst(p.j), self.s.at[slot], self.r.at[p.j], p.mate(da, other))

    def hand(self):
        p, back = self.p, self.p.side - 1
        for lane, origin, way in ((0, p.spot(back), p.mate(1)), (1, p.spot(1), p.mate(back, OTHER))):
            landed(self.relay.at[lane], self.hr.at[lane])
            self.sends(self.relay.at[lane], self.dst(origin), self.fs.at[lane], self.r.at[origin], way)

    def arrived(self, da, other):
        spot = self.p.spot(da, other)
        landed(self.dst(spot), self.r.at[spot])


def dot_nt(a, b):
    return lax.dot_general(a, b, (((1,), (1,)), ((), ())), preferred_element_type=F32)


def project_kernel(side, heads, kv, w_ref, wo_ref, x_ref, cos_ref, sin_ref, na_ref, bo_ref, nr_ref, bq_ref, wr_ref,
                   k_ref, v_ref,
                   qkv_out, xb_out, pack_out, wo_out, kt_out, vt_out,
                   wl, wol, wq, xa, hh, csa, packs, acc, res, kin, vin, kmid, vmid, pass_w, pass_o, pass_x, pass_r,
                   s_wl, s_wol, s_loc, s_a2a, r_a2a, s_o, r_o, s_x, r_x, s_pk, r_pk, s_pv, r_pv,
                   s_plus, r_plus, s_minus, r_minus, s_rfar, r_rfar, s_pair, r_pair,
                   c_plus, d_plus, c_minus, d_minus, c_far, d_far, c_pair, d_pair,
                   s_up, r_up, s_dn, r_dn, s_far, r_far, s_res, r_res, s_in, s_mid,
                   h_w, h_o, h_x, h_r):
    p = Place(side)
    t = Place(side, across=True)
    row = p.row
    back = side - 1
    head = w_ref.shape[1] // (heads + 2 * kv)
    qw = heads // kv * head
    depth = w_ref.shape[0]
    wide = qw + 2 * head
    ow = wol.shape[-1]
    rel = rel_order(side)
    order = send_order(side)
    sends = Sends()

    def take(spot, dst, sem):
        parts = ((spot * qw, qw, 0), (heads * head + spot * head, head, qw),
                 ((heads + kv) * head + spot * head, head, qw + head))
        for start, size, at in parts:
            pltpu.make_async_copy(w_ref.at[:, pl.ds(pl.multiple_of(start, head), size)],
                                  dst.at[:, pl.ds(at, size)], sem).start()

    take(p.j, wq.at[p.b, p.j], s_wl.at[0])
    for k, at in enumerate(rel):
        take(p.spot(*at), wl.at[k], s_wl.at[k + 1])
    pltpu.make_async_copy(x_ref, xa.at[p.j], s_loc.at[0]).start()
    for k, at in enumerate(rel + [(0, SAME)]):
        pltpu.make_async_copy(wo_ref.at[:, pl.ds(pl.multiple_of(t.spot(*at) * ow, head), ow)], wol.at[k],
                              s_wol.at[k]).start()

    depth_in, block = kin.shape[0], kin.shape[1]
    per = k_ref.shape[1] // block
    steps = k_ref.shape[0] * per

    def bring(b, slot):
        r, at = b // per, lax.rem(b, per) * block
        return (pltpu.make_async_copy(k_ref.at[r, pl.ds(at, block)], kin.at[slot], s_in.at[slot]),
                pltpu.make_async_copy(v_ref.at[r, pl.ds(at, block)], vin.at[slot], s_in.at[depth_in + slot]))

    def put(b, slot):
        r, at = b // per, lax.rem(b, per) * block
        return (pltpu.make_async_copy(kmid.at[slot], kt_out.at[r, :, pl.ds(at, block)], s_mid.at[slot]),
                pltpu.make_async_copy(vmid.at[slot], vt_out.at[r, :, pl.ds(at, block)], s_mid.at[depth_in + slot]))

    def turn(b, _):
        slot = lax.rem(b, depth_in)
        for copy in bring(b, slot):
            copy.wait()

        @pl.when(b >= depth_in)
        def _():
            for copy in put(b - depth_in, slot):
                copy.wait()
        kmid[slot] = pltpu.einshape('skd->ksd', kin[slot])
        vmid[slot] = pltpu.einshape('skd->ksd', vin[slot])
        for copy in put(b, slot):
            copy.start()

        @pl.when(b + depth_in < steps)
        def _():
            for copy in bring(b + depth_in, slot):
                copy.start()
        return 0

    done = [0]

    def fill(n):
        n = min(n, steps - done[0])
        if n > 0:
            lax.fori_loop(done[0], done[0] + n, turn, 0)
            done[0] += n

    for b in range(depth_in):
        for copy in bring(b, b):
            copy.start()
    packs[p.b, p.j] = jnp.concatenate(
        [na_ref[...].astype(F32), bo_ref[...].astype(F32), nr_ref[...].astype(F32), bq_ref[...],
         jnp.zeros((2, head), F32), wr_ref[...].astype(F32)], axis=0)
    csa[p.j] = jnp.concatenate([cos_ref[...], sin_ref[...]], axis=-1)

    meet(p.mates() + [t.mate(da, other) for da in range(1, side) for other in BOTH])

    gather = ColumnGather(p, sends, wq, (s_up, r_up), (s_dn, r_dn), (s_far, r_far))
    count = r_plus.shape[0]
    cut = xa.shape[1] // count
    tokens = RowGather(p, sends, lambda spot, k: xa.at[spot, pl.ds(k * cut, cut)], count,
                       (s_plus, r_plus), (s_minus, r_minus), (s_rfar, r_rfar), (s_pair, r_pair))
    turns = d_plus.shape[0]
    cut_cs = csa.shape[1] // turns
    tables = RowGather(p, sends, lambda spot, k: csa.at[spot, pl.ds(k * cut_cs, cut_cs)], turns,
                       (c_plus, d_plus), (c_minus, d_minus), (c_far, d_far), (c_pair, d_pair))
    swap_w = Exchange(p, sends, lambda da, other: wl.at[rel.index((da, other))], lambda spot: wq.at[p.b, spot], pass_w,
                      (s_a2a, r_a2a), (h_w.at[0], h_w.at[1], h_w.at[2]))
    swap_o = Exchange(t, sends, lambda da, other: wol.at[rel.index((da, other))], lambda spot: wo_out.at[spot], pass_o,
                      (s_o, r_o), (h_o.at[0], h_o.at[1], h_o.at[2]))
    swap_x = Exchange(
        t, sends, lambda da, other: xa.at[p.j, :, pl.ds(pl.multiple_of(t.spot(da, other) * ow, head), ow)],
        lambda spot: xb_out.at[spot], pass_x, (s_x, r_x), (h_x.at[0], h_x.at[1], h_x.at[2]))
    swap_r = Exchange(
        p, sends, lambda da, other: res.at[da * CORES + (1 - p.c if other else p.c)],
        lambda spot: qkv_out.at[spot], pass_r, (s_res, r_res), (h_r.at[0], h_r.at[1], h_r.at[2]))
    landed(wq.at[p.b, p.j], s_wl.at[0])
    gather.own(0)
    mine = packs.at[p.b, p.j]
    for k, at in enumerate(rel):
        sends(mine, mine, s_pk.at[k], r_pk.at[p.j], p.mate(*at))
    for at in order:
        landed(wl.at[rel.index(at)], s_wl.at[rel.index(at) + 1])
        swap_w.send(*at)
    for k in range(turns):
        tables.own(k)
    landed(xa.at[p.j], s_loc.at[0])
    tokens.own(0)

    for at in rel:
        landed(packs.at[p.b, p.spot(*at)], r_pk.at[p.spot(*at)])
    pv = packs.at[p.b]
    sends(pv, pv, s_pv.at[0], r_pv.at[0], p.above(1))
    sends(pv, pv, s_pv.at[1], r_pv.at[1], p.above(back))
    for k, at in enumerate(rel):
        swap_w.arrived(*at)
        gather.own(k + 1)
        if k == 0:
            pu = packs.at[p.line(back)]
            landed(pu, r_pv.at[0])
            sends(pu, pu, s_pv.at[2], r_pv.at[2], p.above(1))
        if k == 2:
            swap_w.hand()
            for i in range(1, count):
                tokens.own(i)
        fill(2)
    landed(packs.at[p.line(1)], r_pv.at[1])
    landed(packs.at[p.line(2)], r_pv.at[2])
    for k in range(turns):
        tables.near(k)
    out_pack = pltpu.make_async_copy(packs, pack_out, s_loc.at[2])
    out_pack.start()

    model = xa.shape[-1]

    def norm(spot):
        total = jnp.zeros((xa.shape[1], head), F32)
        for i in range(model // head):
            v = xa[spot, :, i * head:(i + 1) * head].astype(F32)
            total = total + v * v
        inv = lax.rsqrt(jnp.sum(total, axis=-1, keepdims=True) / model + NORM_EPS)
        for i in range(model // head):
            v = xa[spot, :, i * head:(i + 1) * head].astype(F32)
            g = packs[i // row, i % row, 0:1, :]
            hh[spot, :, i * head:(i + 1) * head] = (v * inv * g).astype(BF16)

    span = row * depth

    def part(da, db):
        chip = lax.rem(p.a + da, side)
        rows = hh[pl.ds(chip * CORES, CORES), :, pl.ds(pl.multiple_of(p.line(db) * span, span), span)]
        rows = rows.reshape(CORES * hh.shape[1], span)
        return jnp.dot(rows, wq[p.line(db)].reshape(span, wide), preferred_element_type=F32)

    def bias(m):
        e, k = m // 3, lax.rem(m, 3)
        out = 0.0
        for c in range(CORES):
            d = e * CORES + c
            out = out + packs[d // row, lax.rem(d, row), pl.ds(3 + k, 1), :]
        return out

    lanes = lax.broadcasted_iota(jnp.int32, (1, head), 1)

    def finish(da):
        total = acc[da] + part(da, 2)
        chip = lax.rem(p.a + da, side)
        cs = csa[pl.ds(chip * CORES, CORES)].reshape(CORES * csa.shape[1], head)
        turned = pltpu.roll(cs, head // 2, 1)
        low = lanes < head // 2
        cos = jnp.where(low, cs, turned)
        sin = jnp.where(low, -turned, cs)
        n_q = heads // kv
        for i in range(n_q + 2):
            m = p.j * n_q + i if i < n_q else (heads + p.j if i == n_q else heads + kv + p.j)
            v = total[:, i * head:(i + 1) * head] + bias(m)
            if i <= n_q:
                v = v * cos + pltpu.roll(v, head // 2, 1) * sin
            res[da * CORES:(da + 1) * CORES, :, i * head:(i + 1) * head] = v.astype(BF16).reshape(CORES, -1, head)
        for other in BOTH:
            if da or other:
                swap_r.send(da, other)
        if not da:
            pltpu.make_async_copy(res.at[p.c], qkv_out.at[p.j], r_res.at[p.j]).start()

    norm(p.spot(0))
    tokens.from_pair(0)
    norm(p.spot(0, OTHER))
    for k in range(0, 4):
        gather.near(k)
        fill(2)
    acc[0] = part(0, 0)
    for k in range(count):
        if k % 2 == 0:
            for i in range(4 + k, 4 + k + 2):
                gather.near(i)
            fill(2)
        tokens.near(k)
        fill(2)
    for at in order:
        landed(wol.at[rel.index(at)], s_wol.at[rel.index(at)])
        swap_o.send(*at)
    for at in order:
        swap_x.send(*at)
    for k in range(turns):
        tables.far(k)
    landed(wol.at[row - 1], s_wol.at[row - 1])
    own_o = pltpu.make_async_copy(wol.at[row - 1], wo_out.at[t.j], s_loc.at[1])
    own_o.start()
    own_x = pltpu.make_async_copy(xa.at[p.j, :, pl.ds(pl.multiple_of(t.j * ow, head), ow)], xb_out.at[t.j], s_loc.at[3])
    own_x.start()
    fill(steps)
    acc[0] += part(0, 1)
    acc[0] += part(0, back)
    for da in (back, 1):
        norm(p.spot(da))
        tokens.from_pair(da)
        norm(p.spot(da, OTHER))
        acc[da] = part(da, 0)
        acc[da] += part(da, 1)
        acc[da] += part(da, back)
    for k in range(count):
        tokens.far(k)
    norm(p.spot(2))
    tokens.from_pair(2)
    norm(p.spot(2, OTHER))
    for da in range(side):
        tables.from_pair(da)
    acc[2] = part(2, 0)
    acc[2] += part(2, 1)
    acc[2] += part(2, back)
    for k in range(row):
        gather.far(k)
    finish(2)
    finish(1)
    finish(back)
    swap_r.hand()
    swap_o.hand()
    finish(0)
    swap_x.hand()
    for at in rel:
        swap_o.arrived(*at)
        swap_x.arrived(*at)
    for b in range(steps - depth_in, steps):
        for copy in put(b, b % depth_in):
            copy.wait()
    for i in range(row):
        landed(qkv_out.at[i], r_res.at[i])
    own_o.wait()
    own_x.wait()
    out_pack.wait()
    sends.finish()


def output_kernel(side, kv, len_ref, sink_ref, qkv_ref, kt_ref, vt_ref, wo_ref, xb_ref, packs, own,
                  kb0, kb1, vb0, vb1, sb0, sb1, mb0, mb1, lb0, lb1, oa, wq, xbv, acc, res, pass_r,
                  s_k, s_v, s_loc, s_plus, r_plus, s_minus, r_minus, s_rfar, r_rfar, s_pair, r_pair,
                  s_up, r_up, s_dn, r_dn, s_far, r_far, s_res, r_res, h_r):
    p = Place(side, across=True)
    row = p.row
    back = side - 1
    head = packs.shape[-1]
    depth = wq.shape[2]
    wide = wq.shape[3]
    n_tok = oa.shape[1]
    n_req = kt_ref.shape[0]
    slots = kt_ref.shape[2]
    new = n_tok // n_req
    group = qkv_ref.shape[2] // head - 2
    rows = group * new
    total = n_req * kv
    scale = head ** -0.5 * LOG2E
    block = min(512, slots)
    sends = Sends()
    loads = [pltpu.make_async_copy(wo_ref, wq.at[p.b], s_loc.at[0]),
             pltpu.make_async_copy(xb_ref, xbv, s_loc.at[1])]
    for copy in loads:
        copy.start()

    def fetch(n, which, buf, sem):
        n = jnp.minimum(n, total - 1)
        return pltpu.make_async_copy(which.at[n // kv, lax.rem(n, kv)], buf, sem)

    fetch(0, kt_ref, kb0, s_k.at[0]).start()
    fetch(0, vt_ref, vb0, s_v.at[0]).start()
    fetch(1, kt_ref, kb1, s_k.at[1]).start()
    fetch(1, vt_ref, vb1, s_v.at[1]).start()
    meet(p.mates() + [p.above(1), p.above(back)])
    gather = ColumnGather(p, sends, wq, (s_up, r_up), (s_dn, r_dn), (s_far, r_far))
    count = r_plus.shape[0]
    cuts = count // n_req
    lanes = row * wide // cuts
    tokens = RowGather(
        p, sends, lambda spot, k: oa.at[spot, pl.ds(k // cuts * new, new), pl.ds(k % cuts * lanes, lanes)], count,
        (s_plus, r_plus), (s_minus, r_minus), (s_rfar, r_rfar), (s_pair, r_pair))
    swap_r = Exchange(
        p, sends, lambda da, other: res.at[da * CORES + (1 - p.c if other else p.c)],
        lambda spot: own.at[spot], pass_r, (s_res, r_res), (h_r.at[0], h_r.at[1], h_r.at[2]))
    loads[0].wait()
    for k in range(row):
        gather.own(k)
    loads[1].wait()

    def place(r):
        return pl.ds(pl.multiple_of(r * new, new), new)

    ri = lax.rem(lax.broadcasted_iota(jnp.int32, (rows, head), 0), new)
    ci = lax.broadcasted_iota(jnp.int32, (rows, head), 1)

    def first(n, sb, mb, lb, kb):
        n = jnp.minimum(n, total - 1)
        r, i = n // kv, lax.rem(n, kv)
        q = jnp.concatenate([qkv_ref[i, place(r), g * head:(g + 1) * head] for g in range(group)], axis=0)
        length = len_ref[r]
        kn = qkv_ref[i, place(r), group * head:(group + 1) * head]
        kn = jnp.concatenate([kn, jnp.zeros((head - new, head), BF16)], axis=0)
        s = jnp.where(ri >= ci, dot_nt(q, kn), -1e30)
        sb[:, slots:] = s
        m = s
        for b in range(slots // block):
            s = dot_nt(q, kb[b * block:(b + 1) * block])
            s = jnp.where(b * block + lax.broadcasted_iota(jnp.int32, (1, block), 1) < length, s, -1e30)
            sb[:, b * block:(b + 1) * block] = s
            for k in range(block // head):
                m = jnp.maximum(m, s[:, k * head:(k + 1) * head])
            yield
        m = jnp.max(m, axis=-1, keepdims=True) * scale
        sink = jnp.concatenate([jnp.full((new, head), sink_ref[i * group + g] * LOG2E, F32) for g in range(group)], axis=0)
        m = jnp.maximum(m, sink)
        mb[...] = m
        lb[...] = jnp.exp2(sink - m)

    def second(n, sb, mb, lb, vb):
        r, i = n // kv, lax.rem(n, kv)
        m = mb[...]
        vn = qkv_ref[i, place(r), (group + 1) * head:]
        vn = jnp.concatenate([vn, jnp.zeros((head - new, head), BF16)], axis=0)
        pr = jnp.exp2(sb[:, slots:] * scale - m)
        low = pr
        out = jnp.dot(pr.astype(BF16), vn, preferred_element_type=F32)
        for b in range(slots // block):
            prs = []
            for k in range(block // head):
                at = b * block + k * head
                pr = jnp.exp2(sb[:, at:at + head] * scale - m)
                low = low + pr
                prs.append(pr.astype(BF16))
            out = out + jnp.dot(jnp.concatenate(prs, axis=1), vb[b * block:(b + 1) * block], preferred_element_type=F32)
            yield
        out = (out / (jnp.sum(low, axis=-1, keepdims=True) + lb[...])).astype(BF16)
        for g in range(group):
            at = pl.multiple_of((i * group + g) * head, head)
            oa[p.j, place(r), pl.ds(at, head)] = out[g * new:(g + 1) * new]

    def run(*work):
        work = list(work)
        while work:
            for w in list(work):
                if next(w, w) is w:
                    work.remove(w)

    fetch(0, kt_ref, kb0, s_k.at[0]).wait()
    run(first(0, sb0, mb0, lb0, kb0))
    fetch(2, kt_ref, kb0, s_k.at[0]).start()
    turns = total // 2
    each = turns // count

    def events(h):
        out = []
        if (h + 1) % each == 0:
            out.append((tokens.own, h // each))
        for k in range(count):
            if h == (k + 1) * each + 2:
                out.append((tokens.near, k))
            if h == (k + 1) * each + 4:
                out.append((tokens.far, k))
        if h >= turns // 2:
            for k in range(row):
                if turns // 2 + k // 2 == h:
                    out.append((gather.near, k))
        return out

    def body(h, _):
        n = 2 * h
        fetch(n, vt_ref, vb0, s_v.at[0]).wait()
        fetch(n + 1, kt_ref, kb1, s_k.at[1]).wait()
        run(first(n + 1, sb1, mb1, lb1, kb1), second(n, sb0, mb0, lb0, vb0))
        fetch(n + 2, vt_ref, vb0, s_v.at[0]).start()
        fetch(n + 3, kt_ref, kb1, s_k.at[1]).start()
        fetch(n + 1, vt_ref, vb1, s_v.at[1]).wait()
        fetch(n + 2, kt_ref, kb0, s_k.at[0]).wait()
        run(first(n + 2, sb0, mb0, lb0, kb0), second(n + 1, sb1, mb1, lb1, vb1))
        fetch(n + 3, vt_ref, vb1, s_v.at[1]).start()
        fetch(n + 4, kt_ref, kb0, s_k.at[0]).start()
        for at in range(turns):
            todo = events(at)
            if todo:
                @pl.when(h == at)
                def _():
                    for act, k in todo:
                        act(k)
        return 0

    lax.fori_loop(0, turns, body, 0)
    for which, buf, sem in ((vt_ref, vb0, s_v.at[0]), (vt_ref, vb1, s_v.at[1]), (kt_ref, kb0, s_k.at[0]), (kt_ref, kb1, s_k.at[1])):
        fetch(0, which, buf, sem).wait()
    past = [e for h in range(turns) for e in events(h)]

    def rest(act, k):
        if not any(a == act and i == k for a, i in past):
            act(k)

    def part(da, db):
        chip = lax.rem(p.a + da, side)
        cols = [oa[pl.ds(chip * CORES, CORES), :, pl.ds(pl.multiple_of(p.device(a, p.line(db), 0) * depth, depth), CORES * depth)]
                for a in range(side)]
        lhs = jnp.concatenate([v.reshape(CORES * n_tok, CORES * depth) for v in cols], axis=-1)
        return jnp.dot(lhs, wq[p.line(db)].reshape(row * depth, wide), preferred_element_type=F32)

    def finish(da):
        total = acc[da] + part(da, 2)
        chip = lax.rem(p.a + da, side)
        for i in range(wide // head):
            d = p.j * (wide // head) + i
            b = packs[d // row, lax.rem(d, row), 1:2, :]
            at = pl.ds(i * head, head)
            base = xbv[pl.ds(chip * CORES, CORES), :, at].reshape(-1, head).astype(F32)
            v = base + (total[:, i * head:(i + 1) * head] + b)
            res[da * CORES:(da + 1) * CORES, :, at] = v.astype(BF16).reshape(CORES, -1, head)
        for other in BOTH:
            if da or other:
                swap_r.send(da, other)
        if not da:
            pltpu.make_async_copy(res.at[p.c], own.at[p.j], r_res.at[p.j]).start()

    for k in range(row):
        rest(gather.near, k)
    for k in range(count):
        rest(tokens.near, k)
        if k > 1:
            rest(tokens.far, k - 2)
    for da in (back, 1):
        tokens.from_pair(da)
        acc[da] = part(da, 0)
        acc[da] += part(da, 1)
        acc[da] += part(da, back)
        rest(tokens.far, count - 2 if da == back else count - 1)
    for k in range(row):
        gather.far(k)
    finish(1)
    finish(back)
    tokens.from_pair(2)
    acc[2] = part(2, 0)
    acc[2] += part(2, 1)
    acc[2] += part(2, back)
    finish(2)
    tokens.from_pair(0)
    acc[0] = part(0, 0)
    acc[0] += part(0, 1)
    acc[0] += part(0, back)
    finish(0)
    swap_r.hand()
    for i in range(row):
        landed(own.at[i], r_res.at[i])
    sends.finish()


def close_kernel(own, qkv_ref, packs, br_ref, resid_out, logit_out, k_out, v_out):
    row, n_tok, wide = own.shape
    n_req, experts, new = logit_out.shape
    head = packs.shape[-1]
    model = row * wide
    for r in range(n_req):
        k_out[r] = pltpu.einshape('jtd->tjd', qkv_ref[:, r * new:(r + 1) * new, :head])
        v_out[r] = pltpu.einshape('jtd->tjd', qkv_ref[:, r * new:(r + 1) * new, head:])
    square = jnp.zeros((n_tok, head), F32)
    for i in range(row):
        resid_out[:, i * wide:(i + 1) * wide] = own[i]
        for k in range(wide // head):
            v = own[i, :, k * head:(k + 1) * head].astype(F32)
            square = square + v * v
    inv = lax.rsqrt(jnp.sum(square, axis=-1, keepdims=True) / model + NORM_EPS)
    logits = jnp.zeros((experts, n_tok), F32)
    for i in range(row):
        for k in range(wide // head):
            d = i * (wide // head) + k
            v = own[i, :, k * head:(k + 1) * head].astype(F32)
            g = (v * inv * packs[d // row, d % row, 2:3, :]).astype(BF16)
            w = packs[d // row, d % row, 8:8 + experts, :].astype(BF16)
            logits = logits + dot_nt(w, g)
    logits = logits + br_ref[...]
    for r in range(n_req):
        logit_out[r] = logits[:, r * new:(r + 1) * new]


def dma(*shape):
    return pltpu.SemaphoreType.DMA(shape)


def solution(mesh):
    row_spec = P(('dp', 'fsdp'))
    shard_spec = P('fsdp')
    whole_spec = P()
    n_dev = mesh.shape[AXIS]
    side = math.isqrt(n_dev // CORES)
    row = side * CORES
    hbm = pl.BlockSpec(memory_space=pl.ANY)
    vmem = pl.BlockSpec(memory_space=pltpu.VMEM)
    smem = pl.BlockSpec(memory_space=pltpu.SMEM)

    def local_step(tokens, k_cache, v_cache, prefix_len, rope_cos, rope_sin, norm_attn, w_qkv, b_qkv, sink_logits, w_out, b_out, norm_router, w_router, b_router):
        n_req, n_new, model = tokens.shape
        kv, head = k_cache.shape[2:]
        heads = sink_logits.shape[0]
        experts = b_router.shape[0]
        depth = w_qkv.shape[0]
        n_tok = n_req * n_new
        wide = w_qkv.shape[1] // row
        ow = model // row
        flat = tokens.reshape(n_tok, model)
        core = lax.rem(lax.axis_index(AXIS), CORES)
        bias_pad = lax.dynamic_update_slice(jnp.zeros((3 * head,), F32), b_qkv.astype(F32), (core * b_qkv.shape[0],))
        n_pack = 8 + experts

        pieces = 4
        turn = 256
        slots = k_cache.shape[1]
        qkv, xb, packs, wo, kt, vt = pl.pallas_call(
            functools.partial(project_kernel, side, heads, kv),
            out_shape=(jax.ShapeDtypeStruct((row, n_tok, wide), BF16),
                       jax.ShapeDtypeStruct((row, n_tok, ow), BF16),
                       jax.ShapeDtypeStruct((side, row, n_pack, head), F32),
                       jax.ShapeDtypeStruct((row, depth, ow), BF16),
                       jax.ShapeDtypeStruct((n_req, kv, slots, head), BF16),
                       jax.ShapeDtypeStruct((n_req, kv, slots, head), BF16)),
            in_specs=[hbm, hbm, hbm] + [vmem] * 7 + [hbm, hbm],
            out_specs=(hbm,) * 6,
            scratch_shapes=[
                pltpu.VMEM((row - 1, depth, wide), BF16),
                pltpu.VMEM((row, depth, ow), BF16),
                pltpu.VMEM((side, row, depth, wide), BF16),
                pltpu.VMEM((row, n_tok, model), BF16),
                pltpu.VMEM((row, n_tok, model), BF16),
                pltpu.VMEM((row, n_tok, head), F32),
                pltpu.VMEM((side, row, n_pack, head), F32),
                pltpu.VMEM((side, CORES * n_tok, wide), F32),
                pltpu.VMEM((row, n_tok, wide), BF16),
                *[pltpu.VMEM((pieces, turn, kv, head), BF16)] * 2, *[pltpu.VMEM((pieces, kv, turn, head), BF16)] * 2,
                pltpu.VMEM((2, depth, wide), BF16), *[pltpu.VMEM((2, depth, ow), BF16)] * 2,
                pltpu.VMEM((2, n_tok, wide), BF16),
                *[dma(row)] * 2, dma(pieces), *[dma(row)] * 8, *[dma(side)] * 2,
                *[dma(pieces)] * 6, *[dma(side * pieces)] * 2, *[dma(2)] * 6, *[dma(2 * side)] * 2,
                *[dma(row)] * 8, *[dma(2 * pieces)] * 2, *[dma(3, 2)] * 4],
            compiler_params=pltpu.CompilerParams(collective_id=0, has_side_effects=True, vmem_limit_bytes=60 * 2**20),
            name='project',
        )(w_qkv, w_out, flat, rope_cos.reshape(n_tok, head // 2), rope_sin.reshape(n_tok, head // 2),
          norm_attn.reshape(1, head), b_out.reshape(1, head), norm_router.reshape(1, head),
          bias_pad.reshape(3, head), w_router.T, k_cache, v_cache)

        n_row = heads // kv * n_new
        parts = 4 * n_req
        own = pl.pallas_call(
            functools.partial(output_kernel, side, kv),
            out_shape=jax.ShapeDtypeStruct((row, n_tok, ow), BF16),
            in_specs=[smem, smem, vmem, hbm, hbm, hbm, hbm, vmem],
            out_specs=hbm,
            scratch_shapes=[
                *[pltpu.VMEM((slots, head), BF16)] * 4, *[pltpu.VMEM((n_row, slots + head), F32)] * 2,
                *[pltpu.VMEM((n_row, head), F32)] * 4,
                pltpu.VMEM((row, n_tok, model), BF16),
                pltpu.VMEM((side, row, depth, ow), BF16),
                pltpu.VMEM((row, n_tok, ow), BF16),
                pltpu.VMEM((side, CORES * n_tok, ow), F32),
                pltpu.VMEM((row, n_tok, ow), BF16),
                pltpu.VMEM((2, n_tok, ow), BF16),
                *[dma(2)] * 3, *[dma(parts)] * 6, *[dma(side * parts)] * 2, *[dma(row)] * 8, dma(3, 2)],
            compiler_params=pltpu.CompilerParams(collective_id=1, has_side_effects=True, vmem_limit_bytes=56 * 2**20),
            name='output',
        )(prefix_len, sink_logits, qkv, kt, vt, wo, xb, packs)

        gw = wide - 2 * head
        resid, logits, k_new, v_new = pl.pallas_call(
            close_kernel,
            grid=(1,),
            out_shape=(jax.ShapeDtypeStruct((n_tok, model), BF16), jax.ShapeDtypeStruct((n_req, experts, n_new), F32),
                       jax.ShapeDtypeStruct((n_req, n_new, kv, head), BF16),
                       jax.ShapeDtypeStruct((n_req, n_new, kv, head), BF16)),
            in_specs=[pl.BlockSpec((row, n_tok, ow), lambda i: (0, 0, 0)),
                      pl.BlockSpec((row, n_tok, 2 * head), lambda i: (0, 0, gw // (2 * head))),
                      pl.BlockSpec((side, row, n_pack, head), lambda i: (0, 0, 0, 0)),
                      pl.BlockSpec((experts, 1), lambda i: (0, 0))],
            out_specs=(pl.BlockSpec((n_tok, model), lambda i: (0, 0)), pl.BlockSpec((n_req, experts, n_new), lambda i: (0, 0, 0)),
                       pl.BlockSpec((n_req, n_new, kv, head), lambda i: (0, 0, 0, 0)),
                       pl.BlockSpec((n_req, n_new, kv, head), lambda i: (0, 0, 0, 0))),
            name='close',
        )(own, qkv, packs, b_router.reshape(experts, 1))
        return (resid.reshape(n_req, n_new, model), jnp.transpose(logits, (0, 2, 1)), k_new, v_new)

    in_specs = (row_spec, row_spec, row_spec, row_spec, row_spec, row_spec, shard_spec, shard_spec, shard_spec, whole_spec, shard_spec, shard_spec, shard_spec, shard_spec, whole_spec)
    out_specs = (row_spec, row_spec, row_spec, row_spec)
    return jax.shard_map(local_step, mesh=mesh, in_specs=in_specs, out_specs=out_specs, check_vma=False)
```

```python
import functools
import math

import jax
import jax.numpy as jnp
from jax import lax
from jax.experimental import pallas as pl
from jax.experimental.pallas import tpu as pltpu
from jax.sharding import PartitionSpec as P

NORM_EPS = 1e-5
AXIS = 'fsdp'
CORES = 2
MESH_ID = pl.DeviceIdType.MESH
BF16 = jnp.bfloat16
F32 = jnp.float32
LOG2E = 1.4426950408889634
SAME, OTHER = False, True
BOTH = (SAME, OTHER)


class Place:
    def __init__(self, side, across=False):
        index = lax.axis_index(AXIS)
        self.side, self.across = side, across
        self.row = side * CORES
        self.c = lax.rem(index, CORES)
        x = lax.rem(index // CORES, side)
        y = index // self.row
        self.a, self.b = (y, x) if across else (x, y)
        self.j = self.a * CORES + self.c

    def device(self, a, b, c):
        return (a * self.side + b) * CORES + c if self.across else (b * self.side + a) * CORES + c

    def spot(self, da, other=False):
        core = (1 - self.c) if other else self.c
        return lax.rem(self.a + da, self.side) * CORES + core

    def line(self, db):
        return lax.rem(self.b + db, self.side)

    def mate(self, da, other=False):
        return self.device(lax.rem(self.a + da, self.side), self.b, (1 - self.c) if other else self.c)

    def above(self, db):
        return self.device(self.a, self.line(db), self.c)

    def mates(self):
        return [self.mate(da, other) for da in range(self.side) for other in BOTH if da or other]


class Sends:
    def __init__(self):
        self.started = []

    def __call__(self, src, dst, send_sem, recv_sem, device, later=None):
        pltpu.make_async_remote_copy(
            src_ref=src, dst_ref=dst, send_sem=send_sem, recv_sem=recv_sem,
            device_id={AXIS: device}, device_id_type=MESH_ID).start()
        self.started.append(later or (lambda: (src, send_sem)))

    def finish(self):
        for later in self.started:
            landed(*later())


def landed(ref, sem):
    pltpu.make_async_copy(ref, ref, sem).wait()


def meet(peers):
    barrier = pltpu.get_barrier_semaphore()
    for peer in peers:
        pl.semaphore_signal(barrier, inc=1, device_id={AXIS: peer}, device_id_type=MESH_ID)
    pl.semaphore_wait(barrier, len(peers))


def rel_order(side):
    return [(0, OTHER), (1, SAME), (side - 1, SAME), (1, OTHER), (side - 1, OTHER), (2, SAME), (2, OTHER)]


def send_order(side):
    return [(0, OTHER), (1, SAME), (side - 1, SAME), (2, SAME), (2, OTHER), (1, OTHER), (side - 1, OTHER)]


class RowGather:
    def __init__(self, place, sends, view, count, plus, minus, far, pair):
        self.p, self.sends, self.view, self.count = place, sends, view, count
        self.plus, self.minus, self.far_sems, self.pair_sems = plus, minus, far, pair

    def go(self, spot, k, sems, slot, da, other=False):
        v = self.view(spot, k)
        self.sends(v, v, sems[0].at[slot], sems[1].at[slot], self.p.mate(da, other), lambda: (self.view(0, k), sems[0].at[slot]))

    def own(self, k):
        p = self.p
        self.go(p.j, k, self.plus, k, 1)
        self.go(p.j, k, self.minus, k, p.side - 1)
        self.go(p.j, k, self.pair_sems, k, 0, True)

    def near(self, k):
        p, back, n = self.p, self.p.side - 1, self.count
        low, high = p.spot(back), p.spot(1)
        landed(self.view(low, k), self.plus[1].at[k])
        if k % 2 == 0:
            self.go(low, k, self.far_sems, k, 1)
        self.go(low, k, self.pair_sems, n + k, 0, True)
        landed(self.view(high, k), self.minus[1].at[k])
        if k % 2 == 1:
            self.go(high, k, self.far_sems, k, back)
        self.go(high, k, self.pair_sems, 2 * n + k, 0, True)

    def far(self, k):
        spot = self.p.spot(2)
        landed(self.view(spot, k), self.far_sems[1].at[k])
        self.go(spot, k, self.pair_sems, 3 * self.count + k, 0, True)

    def from_pair(self, da):
        group = {0: 0, self.p.side - 1: 1, 1: 2, 2: 3}[da]
        for k in range(self.count):
            landed(self.view(self.p.spot(da, OTHER), k), self.pair_sems[1].at[group * self.count + k])


class ColumnGather:
    def __init__(self, place, sends, buf, up, down, far):
        self.p, self.sends, self.buf = place, sends, buf
        self.up, self.down, self.far_sems = up, down, far
        self.order = [(0, SAME)] + rel_order(place.side)

    def go(self, line, k, sems, db):
        v = self.buf.at[line, self.p.spot(*self.order[k])]
        self.sends(v, v, sems[0].at[k], sems[1].at[k], self.p.above(db), lambda: (self.buf.at[0, 0], sems[0].at[k]))

    def own(self, k):
        self.go(self.p.b, k, self.up, 1)
        self.go(self.p.b, k, self.down, self.p.side - 1)

    def near(self, k):
        p, back = self.p, self.p.side - 1
        spot = p.spot(*self.order[k])
        landed(self.buf.at[p.line(back), spot], self.up[1].at[k])
        if k % 2 == 0:
            self.go(p.line(back), k, self.far_sems, 1)
        landed(self.buf.at[p.line(1), spot], self.down[1].at[k])
        if k % 2 == 1:
            self.go(p.line(1), k, self.far_sems, back)

    def far(self, k):
        landed(self.buf.at[self.p.line(2), self.p.spot(*self.order[k])], self.far_sems[1].at[k])


class Exchange:
    def __init__(self, place, sends, src, dst, relay, sems, hand_sems):
        self.p, self.sends, self.src, self.dst, self.relay = place, sends, src, dst, relay
        (self.s, self.r), (self.hs, self.hr, self.fs) = sems, hand_sems

    def send(self, da, other):
        p, slot = self.p, da * CORES + other
        if da == 2:
            way = p.side - 1 if other else 1
            self.sends(self.src(da, other), self.relay.at[int(other)], self.hs.at[int(other)], self.hr.at[int(other)],
                       p.mate(way))
        else:
            self.sends(self.src(da, other), self.dst(p.j), self.s.at[slot], self.r.at[p.j], p.mate(da, other))

    def hand(self):
        p, back = self.p, self.p.side - 1
        for lane, origin, way in ((0, p.spot(back), p.mate(1)), (1, p.spot(1), p.mate(back, OTHER))):
            landed(self.relay.at[lane], self.hr.at[lane])
            self.sends(self.relay.at[lane], self.dst(origin), self.fs.at[lane], self.r.at[origin], way)

    def arrived(self, da, other):
        spot = self.p.spot(da, other)
        landed(self.dst(spot), self.r.at[spot])


def dot_nt(a, b):
    return lax.dot_general(a, b, (((1,), (1,)), ((), ())), preferred_element_type=F32)


def project_kernel(side, heads, kv, w_ref, wo_ref, x_ref, cos_ref, sin_ref, na_ref, bo_ref, nr_ref, bq_ref, wr_ref,
                   k_ref, v_ref,
                   qkv_out, xb_out, pack_out, wo_out, kt_out, vt_out,
                   wl, wol, wq, xa, hh, csa, packs, acc, res, kin, vin, kmid, vmid, pass_w, pass_o, pass_x, pass_r,
                   s_wl, s_wol, s_loc, s_a2a, r_a2a, s_o, r_o, s_x, r_x, s_pk, r_pk, s_pv, r_pv,
                   s_plus, r_plus, s_minus, r_minus, s_rfar, r_rfar, s_pair, r_pair,
                   c_plus, d_plus, c_minus, d_minus, c_far, d_far, c_pair, d_pair,
                   s_up, r_up, s_dn, r_dn, s_far, r_far, s_res, r_res, s_in, s_mid,
                   h_w, h_o, h_x, h_r):
    p = Place(side)
    t = Place(side, across=True)
    row = p.row
    back = side - 1
    head = w_ref.shape[1] // (heads + 2 * kv)
    qw = heads // kv * head
    depth = w_ref.shape[0]
    wide = qw + 2 * head
    ow = wol.shape[-1]
    rel = rel_order(side)
    order = send_order(side)
    sends = Sends()

    def take(spot, dst, sem):
        parts = ((spot * qw, qw, 0), (heads * head + spot * head, head, qw),
                 ((heads + kv) * head + spot * head, head, qw + head))
        for start, size, at in parts:
            pltpu.make_async_copy(w_ref.at[:, pl.ds(pl.multiple_of(start, head), size)],
                                  dst.at[:, pl.ds(at, size)], sem).start()

    take(p.j, wq.at[p.b, p.j], s_wl.at[0])
    for k, at in enumerate(rel):
        take(p.spot(*at), wl.at[k], s_wl.at[k + 1])
    pltpu.make_async_copy(x_ref, xa.at[p.j], s_loc.at[0]).start()
    for k, at in enumerate(rel + [(0, SAME)]):
        pltpu.make_async_copy(wo_ref.at[:, pl.ds(pl.multiple_of(t.spot(*at) * ow, head), ow)], wol.at[k],
                              s_wol.at[k]).start()

    depth_in, block = kin.shape[0], kin.shape[1]
    per = k_ref.shape[1] // block
    steps = k_ref.shape[0] * per

    def bring(b, slot):
        r, at = b // per, lax.rem(b, per) * block
        return (pltpu.make_async_copy(k_ref.at[r, pl.ds(at, block)], kin.at[slot], s_in.at[slot]),
                pltpu.make_async_copy(v_ref.at[r, pl.ds(at, block)], vin.at[slot], s_in.at[depth_in + slot]))

    def put(b, slot):
        r, at = b // per, lax.rem(b, per) * block
        return (pltpu.make_async_copy(kmid.at[slot], kt_out.at[r, :, pl.ds(at, block)], s_mid.at[slot]),
                pltpu.make_async_copy(vmid.at[slot], vt_out.at[r, :, pl.ds(at, block)], s_mid.at[depth_in + slot]))

    def turn(b, _):
        slot = lax.rem(b, depth_in)
        for copy in bring(b, slot):
            copy.wait()

        @pl.when(b >= depth_in)
        def _():
            for copy in put(b - depth_in, slot):
                copy.wait()
        kmid[slot] = pltpu.einshape('skd->ksd', kin[slot])
        vmid[slot] = pltpu.einshape('skd->ksd', vin[slot])
        for copy in put(b, slot):
            copy.start()

        @pl.when(b + depth_in < steps)
        def _():
            for copy in bring(b + depth_in, slot):
                copy.start()
        return 0

    done = [0]

    def fill(n):
        n = min(n, steps - done[0])
        if n > 0:
            lax.fori_loop(done[0], done[0] + n, turn, 0)
            done[0] += n

    for b in range(depth_in):
        for copy in bring(b, b):
            copy.start()
    packs[p.b, p.j] = jnp.concatenate(
        [na_ref[...].astype(F32), bo_ref[...].astype(F32), nr_ref[...].astype(F32), bq_ref[...],
         jnp.zeros((2, head), F32), wr_ref[...].astype(F32)], axis=0)
    csa[p.j] = jnp.concatenate([cos_ref[...], sin_ref[...]], axis=-1)

    meet(p.mates() + [t.mate(da, other) for da in range(1, side) for other in BOTH])

    gather = ColumnGather(p, sends, wq, (s_up, r_up), (s_dn, r_dn), (s_far, r_far))
    count = r_plus.shape[0]
    cut = xa.shape[1] // count
    tokens = RowGather(p, sends, lambda spot, k: xa.at[spot, pl.ds(k * cut, cut)], count,
                       (s_plus, r_plus), (s_minus, r_minus), (s_rfar, r_rfar), (s_pair, r_pair))
    turns = d_plus.shape[0]
    cut_cs = csa.shape[1] // turns
    tables = RowGather(p, sends, lambda spot, k: csa.at[spot, pl.ds(k * cut_cs, cut_cs)], turns,
                       (c_plus, d_plus), (c_minus, d_minus), (c_far, d_far), (c_pair, d_pair))
    swap_w = Exchange(p, sends, lambda da, other: wl.at[rel.index((da, other))], lambda spot: wq.at[p.b, spot], pass_w,
                      (s_a2a, r_a2a), (h_w.at[0], h_w.at[1], h_w.at[2]))
    swap_o = Exchange(t, sends, lambda da, other: wol.at[rel.index((da, other))], lambda spot: wo_out.at[spot], pass_o,
                      (s_o, r_o), (h_o.at[0], h_o.at[1], h_o.at[2]))
    swap_x = Exchange(
        t, sends, lambda da, other: xa.at[p.j, :, pl.ds(pl.multiple_of(t.spot(da, other) * ow, head), ow)],
        lambda spot: xb_out.at[spot], pass_x, (s_x, r_x), (h_x.at[0], h_x.at[1], h_x.at[2]))
    swap_r = Exchange(
        p, sends, lambda da, other: res.at[da * CORES + (1 - p.c if other else p.c)],
        lambda spot: qkv_out.at[spot], pass_r, (s_res, r_res), (h_r.at[0], h_r.at[1], h_r.at[2]))
    landed(wq.at[p.b, p.j], s_wl.at[0])
    gather.own(0)
    mine = packs.at[p.b, p.j]
    for k, at in enumerate(rel):
        sends(mine, mine, s_pk.at[k], r_pk.at[p.j], p.mate(*at))
    for at in order:
        landed(wl.at[rel.index(at)], s_wl.at[rel.index(at) + 1])
        swap_w.send(*at)
    for k in range(turns):
        tables.own(k)
    landed(xa.at[p.j], s_loc.at[0])
    tokens.own(0)

    for at in rel:
        landed(packs.at[p.b, p.spot(*at)], r_pk.at[p.spot(*at)])
    pv = packs.at[p.b]
    sends(pv, pv, s_pv.at[0], r_pv.at[0], p.above(1))
    sends(pv, pv, s_pv.at[1], r_pv.at[1], p.above(back))
    for k, at in enumerate(rel):
        swap_w.arrived(*at)
        gather.own(k + 1)
        if k == 0:
            pu = packs.at[p.line(back)]
            landed(pu, r_pv.at[0])
            sends(pu, pu, s_pv.at[2], r_pv.at[2], p.above(1))
        if k == 2:
            swap_w.hand()
            for i in range(1, count):
                tokens.own(i)
        fill(2)
    landed(packs.at[p.line(1)], r_pv.at[1])
    landed(packs.at[p.line(2)], r_pv.at[2])
    for k in range(turns):
        tables.near(k)
    out_pack = pltpu.make_async_copy(packs, pack_out, s_loc.at[2])
    out_pack.start()

    model = xa.shape[-1]

    def norm(spot):
        total = jnp.zeros((xa.shape[1], head), F32)
        for i in range(model // head):
            v = xa[spot, :, i * head:(i + 1) * head].astype(F32)
            total = total + v * v
        inv = lax.rsqrt(jnp.sum(total, axis=-1, keepdims=True) / model + NORM_EPS)
        for i in range(model // head):
            v = xa[spot, :, i * head:(i + 1) * head].astype(F32)
            g = packs[i // row, i % row, 0:1, :]
            hh[spot, :, i * head:(i + 1) * head] = (v * inv * g).astype(BF16)

    span = row * depth

    def part(da, db):
        chip = lax.rem(p.a + da, side)
        rows = hh[pl.ds(chip * CORES, CORES), :, pl.ds(pl.multiple_of(p.line(db) * span, span), span)]
        rows = rows.reshape(CORES * hh.shape[1], span)
        return jnp.dot(rows, wq[p.line(db)].reshape(span, wide), preferred_element_type=F32)

    def bias(m):
        e, k = m // 3, lax.rem(m, 3)
        out = 0.0
        for c in range(CORES):
            d = e * CORES + c
            out = out + packs[d // row, lax.rem(d, row), pl.ds(3 + k, 1), :]
        return out

    lanes = lax.broadcasted_iota(jnp.int32, (1, head), 1)

    def finish(da):
        total = acc[da] + part(da, 2)
        chip = lax.rem(p.a + da, side)
        cs = csa[pl.ds(chip * CORES, CORES)].reshape(CORES * csa.shape[1], head)
        turned = pltpu.roll(cs, head // 2, 1)
        low = lanes < head // 2
        cos = jnp.where(low, cs, turned)
        sin = jnp.where(low, -turned, cs)
        n_q = heads // kv
        for i in range(n_q + 2):
            m = p.j * n_q + i if i < n_q else (heads + p.j if i == n_q else heads + kv + p.j)
            v = total[:, i * head:(i + 1) * head] + bias(m)
            if i <= n_q:
                v = v * cos + pltpu.roll(v, head // 2, 1) * sin
            res[da * CORES:(da + 1) * CORES, :, i * head:(i + 1) * head] = v.astype(BF16).reshape(CORES, -1, head)
        for other in BOTH:
            if da or other:
                swap_r.send(da, other)
        if not da:
            pltpu.make_async_copy(res.at[p.c], qkv_out.at[p.j], r_res.at[p.j]).start()

    norm(p.spot(0))
    tokens.from_pair(0)
    norm(p.spot(0, OTHER))
    for k in range(0, 4):
        gather.near(k)
        fill(2)
    acc[0] = part(0, 0)
    for k in range(count):
        if k % 2 == 0:
            for i in range(4 + k, 4 + k + 2):
                gather.near(i)
            fill(2)
        tokens.near(k)
        fill(2)
    for at in order:
        landed(wol.at[rel.index(at)], s_wol.at[rel.index(at)])
        swap_o.send(*at)
    for at in order:
        swap_x.send(*at)
    for k in range(turns):
        tables.far(k)
    landed(wol.at[row - 1], s_wol.at[row - 1])
    own_o = pltpu.make_async_copy(wol.at[row - 1], wo_out.at[t.j], s_loc.at[1])
    own_o.start()
    own_x = pltpu.make_async_copy(xa.at[p.j, :, pl.ds(pl.multiple_of(t.j * ow, head), ow)], xb_out.at[t.j], s_loc.at[3])
    own_x.start()
    fill(steps)
    acc[0] += part(0, 1)
    acc[0] += part(0, back)
    for da in (back, 1):
        norm(p.spot(da))
        tokens.from_pair(da)
        norm(p.spot(da, OTHER))
        acc[da] = part(da, 0)
        acc[da] += part(da, 1)
        acc[da] += part(da, back)
    for da in range(side):
        tables.from_pair(da)
    for k in range(count // 2):
        tokens.far(k)
    for k in range(row):
        gather.far(k)
    finish(1)
    finish(back)
    for k in range(count // 2, count):
        tokens.far(k)
    norm(p.spot(2))
    tokens.from_pair(2)
    norm(p.spot(2, OTHER))
    acc[2] = part(2, 0)
    acc[2] += part(2, 1)
    acc[2] += part(2, back)
    finish(2)
    swap_o.hand()
    finish(0)
    swap_x.hand()
    swap_r.hand()
    for at in rel:
        swap_o.arrived(*at)
        swap_x.arrived(*at)
    for b in range(steps - depth_in, steps):
        for copy in put(b, b % depth_in):
            copy.wait()
    for i in range(row):
        landed(qkv_out.at[i], r_res.at[i])
    own_o.wait()
    own_x.wait()
    out_pack.wait()
    sends.finish()


def output_kernel(side, kv, len_ref, sink_ref, qkv_ref, kt_ref, vt_ref, wo_ref, xb_ref, packs, own,
                  kb, vb, sb0, sb1, mb0, mb1, lb0, lb1, oa, wq, xbv, acc, res, pass_r,
                  s_k, s_v, s_loc, s_plus, r_plus, s_minus, r_minus, s_rfar, r_rfar, s_pair, r_pair,
                  s_up, r_up, s_dn, r_dn, s_far, r_far, s_res, r_res, h_r):
    p = Place(side, across=True)
    row = p.row
    back = side - 1
    head = packs.shape[-1]
    depth = wq.shape[2]
    wide = wq.shape[3]
    n_tok = oa.shape[1]
    n_req = kt_ref.shape[0]
    slots = kt_ref.shape[2]
    new = n_tok // n_req
    group = qkv_ref.shape[2] // head - 2
    rows = group * new
    total = n_req * kv
    scale = head ** -0.5 * LOG2E
    block = min(512, slots)
    sends = Sends()
    loads = [pltpu.make_async_copy(wo_ref, wq.at[p.b], s_loc.at[0]),
             pltpu.make_async_copy(xb_ref, xbv, s_loc.at[1])]
    for copy in loads:
        copy.start()

    deep = kb.shape[0]
    quarter = slots // deep

    def fetch(n, which, buf, sem):
        slot = lax.rem(n, deep)

        @pl.when(n < total)
        def _():
            for k in range(deep):
                at = pl.ds(k * quarter, quarter)
                pltpu.make_async_copy(which.at[n // kv, lax.rem(n, kv), at], buf.at[slot, at], sem.at[slot]).start()

    def fetched(n, buf, sem):
        slot = lax.rem(n, deep)

        @pl.when(n < total)
        def _():
            landed(buf.at[slot], sem.at[slot])

    for n in range(deep):
        fetch(jnp.int32(n), kt_ref, kb, s_k)
        fetch(jnp.int32(n), vt_ref, vb, s_v)
    meet(p.mates() + [p.above(1), p.above(back)])
    gather = ColumnGather(p, sends, wq, (s_up, r_up), (s_dn, r_dn), (s_far, r_far))
    count = r_plus.shape[0]
    cuts = count // n_req
    lanes = row * wide // cuts
    tokens = RowGather(
        p, sends, lambda spot, k: oa.at[spot, pl.ds(k // cuts * new, new), pl.ds(k % cuts * lanes, lanes)], count,
        (s_plus, r_plus), (s_minus, r_minus), (s_rfar, r_rfar), (s_pair, r_pair))
    swap_r = Exchange(
        p, sends, lambda da, other: res.at[da * CORES + (1 - p.c if other else p.c)],
        lambda spot: own.at[spot], pass_r, (s_res, r_res), (h_r.at[0], h_r.at[1], h_r.at[2]))
    loads[0].wait()
    for k in range(row):
        gather.own(k)
    loads[1].wait()

    def place(r):
        return pl.ds(pl.multiple_of(r * new, new), new)

    ri = lax.rem(lax.broadcasted_iota(jnp.int32, (rows, head), 0), new)
    ci = lax.broadcasted_iota(jnp.int32, (rows, head), 1)

    def first(n, sb, mb, lb):
        slot = lax.rem(n, deep)
        n = jnp.minimum(n, total - 1)
        r, i = n // kv, lax.rem(n, kv)
        q = jnp.concatenate([qkv_ref[i, place(r), g * head:(g + 1) * head] for g in range(group)], axis=0)
        length = len_ref[r]
        kn = qkv_ref[i, place(r), group * head:(group + 1) * head]
        kn = jnp.concatenate([kn, jnp.zeros((head - new, head), BF16)], axis=0)
        s = jnp.where(ri >= ci, dot_nt(q, kn), -1e30)
        sb[:, slots:] = s
        m = s
        for b in range(slots // block):
            s = dot_nt(q, kb[slot, b * block:(b + 1) * block])
            s = jnp.where(b * block + lax.broadcasted_iota(jnp.int32, (1, block), 1) < length, s, -1e30)
            sb[:, b * block:(b + 1) * block] = s
            for k in range(block // head):
                m = jnp.maximum(m, s[:, k * head:(k + 1) * head])
            yield
        m = jnp.max(m, axis=-1, keepdims=True) * scale
        sink = jnp.concatenate([jnp.full((new, head), sink_ref[i * group + g] * LOG2E, F32) for g in range(group)], axis=0)
        m = jnp.maximum(m, sink)
        mb[...] = m
        lb[...] = jnp.exp2(sink - m)

    def second(n, sb, mb, lb):
        slot = lax.rem(n, deep)
        r, i = n // kv, lax.rem(n, kv)
        m = mb[...]
        vn = qkv_ref[i, place(r), (group + 1) * head:]
        vn = jnp.concatenate([vn, jnp.zeros((head - new, head), BF16)], axis=0)
        pr = jnp.exp2(sb[:, slots:] * scale - m)
        low = pr
        out = jnp.dot(pr.astype(BF16), vn, preferred_element_type=F32)
        for b in range(slots // block):
            prs = []
            for k in range(block // head):
                at = b * block + k * head
                pr = jnp.exp2(sb[:, at:at + head] * scale - m)
                low = low + pr
                prs.append(pr.astype(BF16))
            out = out + jnp.dot(jnp.concatenate(prs, axis=1), vb[slot, b * block:(b + 1) * block], preferred_element_type=F32)
            yield
        out = (out / (jnp.sum(low, axis=-1, keepdims=True) + lb[...])).astype(BF16)
        for g in range(group):
            at = pl.multiple_of((i * group + g) * head, head)
            oa[p.j, place(r), pl.ds(at, head)] = out[g * new:(g + 1) * new]

    def run(*work):
        work = list(work)
        while work:
            for w in list(work):
                if next(w, w) is w:
                    work.remove(w)

    fetched(jnp.int32(0), kb, s_k)
    run(first(jnp.int32(0), sb0, mb0, lb0))
    fetch(jnp.int32(deep), kt_ref, kb, s_k)
    turns = total // 2
    each = turns // count

    def events(h):
        out = []
        if (h + 1) % each == 0:
            out.append((tokens.own, h // each))
        for k in range(count):
            if h == (k + 1) * each + 2:
                out.append((tokens.near, k))
            if h == (k + 1) * each + 4:
                out.append((tokens.far, k))
        if h >= turns // 2:
            for k in range(row):
                if turns // 2 + k // 2 == h:
                    out.append((gather.near, k))
        return out

    def body(h, _):
        for n, one, two in ((2 * h, (sb1, mb1, lb1), (sb0, mb0, lb0)), (2 * h + 1, (sb0, mb0, lb0), (sb1, mb1, lb1))):
            fetched(n, vb, s_v)
            fetched(n + 1, kb, s_k)
            run(first(n + 1, *one), second(n, *two))
            fetch(n + deep, vt_ref, vb, s_v)
            fetch(n + deep + 1, kt_ref, kb, s_k)
        for at in range(turns):
            todo = events(at)
            if todo:
                @pl.when(h == at)
                def _():
                    for act, k in todo:
                        act(k)
        return 0

    lax.fori_loop(0, turns, body, 0)
    past = [e for h in range(turns) for e in events(h)]

    def rest(act, k):
        if not any(a == act and i == k for a, i in past):
            act(k)

    def part(da, db):
        chip = lax.rem(p.a + da, side)
        cols = [oa[pl.ds(chip * CORES, CORES), :, pl.ds(pl.multiple_of(p.device(a, p.line(db), 0) * depth, depth), CORES * depth)]
                for a in range(side)]
        lhs = jnp.concatenate([v.reshape(CORES * n_tok, CORES * depth) for v in cols], axis=-1)
        return jnp.dot(lhs, wq[p.line(db)].reshape(row * depth, wide), preferred_element_type=F32)

    def finish(da):
        total = acc[da] + part(da, 2)
        chip = lax.rem(p.a + da, side)
        for i in range(wide // head):
            d = p.j * (wide // head) + i
            b = packs[d // row, lax.rem(d, row), 1:2, :]
            at = pl.ds(i * head, head)
            base = xbv[pl.ds(chip * CORES, CORES), :, at].reshape(-1, head).astype(F32)
            v = base + (total[:, i * head:(i + 1) * head] + b)
            res[da * CORES:(da + 1) * CORES, :, at] = v.astype(BF16).reshape(CORES, -1, head)
        for other in BOTH:
            if da or other:
                swap_r.send(da, other)
        if not da:
            pltpu.make_async_copy(res.at[p.c], own.at[p.j], r_res.at[p.j]).start()

    for k in range(row):
        rest(gather.near, k)
    for k in range(count):
        rest(tokens.near, k)
        if k > 1:
            rest(tokens.far, k - 2)
    for da in (back, 1):
        tokens.from_pair(da)
        acc[da] = part(da, 0)
        acc[da] += part(da, 1)
        acc[da] += part(da, back)
        rest(tokens.far, count - 2 if da == back else count - 1)
    for k in range(row):
        gather.far(k)
    finish(1)
    finish(back)
    tokens.from_pair(2)
    acc[2] = part(2, 0)
    acc[2] += part(2, 1)
    acc[2] += part(2, back)
    finish(2)
    tokens.from_pair(0)
    acc[0] = part(0, 0)
    acc[0] += part(0, 1)
    acc[0] += part(0, back)
    finish(0)
    swap_r.hand()
    for i in range(row):
        landed(own.at[i], r_res.at[i])
    sends.finish()


def close_kernel(own, qkv_ref, packs, br_ref, resid_out, logit_out, k_out, v_out):
    row, n_tok, wide = own.shape
    n_req, experts, new = logit_out.shape
    head = packs.shape[-1]
    model = row * wide
    for r in range(n_req):
        k_out[r] = pltpu.einshape('jtd->tjd', qkv_ref[:, r * new:(r + 1) * new, :head])
        v_out[r] = pltpu.einshape('jtd->tjd', qkv_ref[:, r * new:(r + 1) * new, head:])
    square = jnp.zeros((n_tok, head), F32)
    for i in range(row):
        resid_out[:, i * wide:(i + 1) * wide] = own[i]
        for k in range(wide // head):
            v = own[i, :, k * head:(k + 1) * head].astype(F32)
            square = square + v * v
    inv = lax.rsqrt(jnp.sum(square, axis=-1, keepdims=True) / model + NORM_EPS)
    logits = jnp.zeros((experts, n_tok), F32)
    for i in range(row):
        for k in range(wide // head):
            d = i * (wide // head) + k
            v = own[i, :, k * head:(k + 1) * head].astype(F32)
            g = (v * inv * packs[d // row, d % row, 2:3, :]).astype(BF16)
            w = packs[d // row, d % row, 8:8 + experts, :].astype(BF16)
            logits = logits + dot_nt(w, g)
    logits = logits + br_ref[...]
    for r in range(n_req):
        logit_out[r] = logits[:, r * new:(r + 1) * new]


def dma(*shape):
    return pltpu.SemaphoreType.DMA(shape)


def solution(mesh):
    row_spec = P(('dp', 'fsdp'))
    shard_spec = P('fsdp')
    whole_spec = P()
    n_dev = mesh.shape[AXIS]
    side = math.isqrt(n_dev // CORES)
    row = side * CORES
    hbm = pl.BlockSpec(memory_space=pl.ANY)
    vmem = pl.BlockSpec(memory_space=pltpu.VMEM)
    smem = pl.BlockSpec(memory_space=pltpu.SMEM)

    def local_step(tokens, k_cache, v_cache, prefix_len, rope_cos, rope_sin, norm_attn, w_qkv, b_qkv, sink_logits, w_out, b_out, norm_router, w_router, b_router):
        n_req, n_new, model = tokens.shape
        kv, head = k_cache.shape[2:]
        heads = sink_logits.shape[0]
        experts = b_router.shape[0]
        depth = w_qkv.shape[0]
        n_tok = n_req * n_new
        wide = w_qkv.shape[1] // row
        ow = model // row
        flat = tokens.reshape(n_tok, model)
        core = lax.rem(lax.axis_index(AXIS), CORES)
        bias_pad = lax.dynamic_update_slice(jnp.zeros((3 * head,), F32), b_qkv.astype(F32), (core * b_qkv.shape[0],))
        n_pack = 8 + experts

        pieces = 4
        turn = 256
        slots = k_cache.shape[1]
        qkv, xb, packs, wo, kt, vt = pl.pallas_call(
            functools.partial(project_kernel, side, heads, kv),
            out_shape=(jax.ShapeDtypeStruct((row, n_tok, wide), BF16),
                       jax.ShapeDtypeStruct((row, n_tok, ow), BF16),
                       jax.ShapeDtypeStruct((side, row, n_pack, head), F32),
                       jax.ShapeDtypeStruct((row, depth, ow), BF16),
                       jax.ShapeDtypeStruct((n_req, kv, slots, head), BF16),
                       jax.ShapeDtypeStruct((n_req, kv, slots, head), BF16)),
            in_specs=[hbm, hbm, hbm] + [vmem] * 7 + [hbm, hbm],
            out_specs=(hbm,) * 6,
            scratch_shapes=[
                pltpu.VMEM((row - 1, depth, wide), BF16),
                pltpu.VMEM((row, depth, ow), BF16),
                pltpu.VMEM((side, row, depth, wide), BF16),
                pltpu.VMEM((row, n_tok, model), BF16),
                pltpu.VMEM((row, n_tok, model), BF16),
                pltpu.VMEM((row, n_tok, head), F32),
                pltpu.VMEM((side, row, n_pack, head), F32),
                pltpu.VMEM((side, CORES * n_tok, wide), F32),
                pltpu.VMEM((row, n_tok, wide), BF16),
                *[pltpu.VMEM((pieces, turn, kv, head), BF16)] * 2, *[pltpu.VMEM((pieces, kv, turn, head), BF16)] * 2,
                pltpu.VMEM((2, depth, wide), BF16), *[pltpu.VMEM((2, depth, ow), BF16)] * 2,
                pltpu.VMEM((2, n_tok, wide), BF16),
                *[dma(row)] * 2, dma(pieces), *[dma(row)] * 8, *[dma(side)] * 2,
                *[dma(pieces)] * 6, *[dma(side * pieces)] * 2, *[dma(2)] * 6, *[dma(2 * side)] * 2,
                *[dma(row)] * 8, *[dma(2 * pieces)] * 2, *[dma(3, 2)] * 4],
            compiler_params=pltpu.CompilerParams(collective_id=0, has_side_effects=True, vmem_limit_bytes=60 * 2**20),
            name='project',
        )(w_qkv, w_out, flat, rope_cos.reshape(n_tok, head // 2), rope_sin.reshape(n_tok, head // 2),
          norm_attn.reshape(1, head), b_out.reshape(1, head), norm_router.reshape(1, head),
          bias_pad.reshape(3, head), w_router.T, k_cache, v_cache)

        n_row = heads // kv * n_new
        parts = 4 * n_req
        own = pl.pallas_call(
            functools.partial(output_kernel, side, kv),
            out_shape=jax.ShapeDtypeStruct((row, n_tok, ow), BF16),
            in_specs=[smem, smem, vmem, hbm, hbm, hbm, hbm, vmem],
            out_specs=hbm,
            scratch_shapes=[
                *[pltpu.VMEM((4, slots, head), BF16)] * 2, *[pltpu.VMEM((n_row, slots + head), F32)] * 2,
                *[pltpu.VMEM((n_row, head), F32)] * 4,
                pltpu.VMEM((row, n_tok, model), BF16),
                pltpu.VMEM((side, row, depth, ow), BF16),
                pltpu.VMEM((row, n_tok, ow), BF16),
                pltpu.VMEM((side, CORES * n_tok, ow), F32),
                pltpu.VMEM((row, n_tok, ow), BF16),
                pltpu.VMEM((2, n_tok, ow), BF16),
                *[dma(4)] * 2, dma(2), *[dma(parts)] * 6, *[dma(side * parts)] * 2, *[dma(row)] * 8, dma(3, 2)],
            compiler_params=pltpu.CompilerParams(collective_id=1, has_side_effects=True, vmem_limit_bytes=56 * 2**20),
            name='output',
        )(prefix_len, sink_logits, qkv, kt, vt, wo, xb, packs)

        gw = wide - 2 * head
        resid, logits, k_new, v_new = pl.pallas_call(
            close_kernel,
            grid=(1,),
            out_shape=(jax.ShapeDtypeStruct((n_tok, model), BF16), jax.ShapeDtypeStruct((n_req, experts, n_new), F32),
                       jax.ShapeDtypeStruct((n_req, n_new, kv, head), BF16),
                       jax.ShapeDtypeStruct((n_req, n_new, kv, head), BF16)),
            in_specs=[pl.BlockSpec((row, n_tok, ow), lambda i: (0, 0, 0)),
                      pl.BlockSpec((row, n_tok, 2 * head), lambda i: (0, 0, gw // (2 * head))),
                      pl.BlockSpec((side, row, n_pack, head), lambda i: (0, 0, 0, 0)),
                      pl.BlockSpec((experts, 1), lambda i: (0, 0))],
            out_specs=(pl.BlockSpec((n_tok, model), lambda i: (0, 0)), pl.BlockSpec((n_req, experts, n_new), lambda i: (0, 0, 0)),
                       pl.BlockSpec((n_req, n_new, kv, head), lambda i: (0, 0, 0, 0)),
                       pl.BlockSpec((n_req, n_new, kv, head), lambda i: (0, 0, 0, 0))),
            name='close',
        )(own, qkv, packs, b_router.reshape(experts, 1))
        return (resid.reshape(n_req, n_new, model), jnp.transpose(logits, (0, 2, 1)), k_new, v_new)

    in_specs = (row_spec, row_spec, row_spec, row_spec, row_spec, row_spec, shard_spec, shard_spec, shard_spec, whole_spec, shard_spec, shard_spec, shard_spec, shard_spec, whole_spec)
    out_specs = (row_spec, row_spec, row_spec, row_spec)
    return jax.shard_map(local_step, mesh=mesh, in_specs=in_specs, out_specs=out_specs, check_vma=False)
```

```python
import functools
import math

import jax
import jax.numpy as jnp
from jax import lax
from jax.experimental import pallas as pl
from jax.experimental.pallas import tpu as pltpu
from jax.sharding import PartitionSpec as P

NORM_EPS = 1e-5
AXIS = 'fsdp'
CORES = 2
MESH_ID = pl.DeviceIdType.MESH
BF16 = jnp.bfloat16
F32 = jnp.float32
LOG2E = 1.4426950408889634
SAME, OTHER = False, True
BOTH = (SAME, OTHER)


class Place:
    def __init__(self, side, across=False):
        index = lax.axis_index(AXIS)
        self.side, self.across = side, across
        self.row = side * CORES
        self.c = lax.rem(index, CORES)
        x = lax.rem(index // CORES, side)
        y = index // self.row
        self.a, self.b = (y, x) if across else (x, y)
        self.j = self.a * CORES + self.c

    def device(self, a, b, c):
        return (a * self.side + b) * CORES + c if self.across else (b * self.side + a) * CORES + c

    def spot(self, da, other=False):
        core = (1 - self.c) if other else self.c
        return lax.rem(self.a + da, self.side) * CORES + core

    def line(self, db):
        return lax.rem(self.b + db, self.side)

    def mate(self, da, other=False):
        return self.device(lax.rem(self.a + da, self.side), self.b, (1 - self.c) if other else self.c)

    def above(self, db):
        return self.device(self.a, self.line(db), self.c)

    def mates(self):
        return [self.mate(da, other) for da in range(self.side) for other in BOTH if da or other]


class Sends:
    def __init__(self):
        self.started = []

    def __call__(self, src, dst, send_sem, recv_sem, device, later=None):
        pltpu.make_async_remote_copy(
            src_ref=src, dst_ref=dst, send_sem=send_sem, recv_sem=recv_sem,
            device_id={AXIS: device}, device_id_type=MESH_ID).start()
        self.started.append(later or (lambda: (src, send_sem)))

    def finish(self):
        for later in self.started:
            landed(*later())


def landed(ref, sem):
    pltpu.make_async_copy(ref, ref, sem).wait()


def meet(peers):
    barrier = pltpu.get_barrier_semaphore()
    for peer in peers:
        pl.semaphore_signal(barrier, inc=1, device_id={AXIS: peer}, device_id_type=MESH_ID)
    pl.semaphore_wait(barrier, len(peers))


def rel_order(side):
    return [(0, OTHER), (1, SAME), (side - 1, SAME), (1, OTHER), (side - 1, OTHER), (2, SAME), (2, OTHER)]


def send_order(side):
    return [(0, OTHER), (1, SAME), (side - 1, SAME), (2, SAME), (2, OTHER), (1, OTHER), (side - 1, OTHER)]


class RowGather:
    def __init__(self, place, sends, view, count, plus, minus, far, pair):
        self.p, self.sends, self.view, self.count = place, sends, view, count
        self.plus, self.minus, self.far_sems, self.pair_sems = plus, minus, far, pair

    def go(self, spot, k, sems, slot, da, other=False):
        v = self.view(spot, k)
        self.sends(v, v, sems[0].at[slot], sems[1].at[slot], self.p.mate(da, other), lambda: (self.view(0, k), sems[0].at[slot]))

    def own(self, k):
        p = self.p
        self.go(p.j, k, self.plus, k, 1)
        self.go(p.j, k, self.minus, k, p.side - 1)
        self.go(p.j, k, self.pair_sems, k, 0, True)

    def near(self, k):
        p, back, n = self.p, self.p.side - 1, self.count
        low, high = p.spot(back), p.spot(1)
        landed(self.view(low, k), self.plus[1].at[k])
        if k % 2 == 0:
            self.go(low, k, self.far_sems, k, 1)
        self.go(low, k, self.pair_sems, n + k, 0, True)
        landed(self.view(high, k), self.minus[1].at[k])
        if k % 2 == 1:
            self.go(high, k, self.far_sems, k, back)
        self.go(high, k, self.pair_sems, 2 * n + k, 0, True)

    def far(self, k):
        spot = self.p.spot(2)
        landed(self.view(spot, k), self.far_sems[1].at[k])
        self.go(spot, k, self.pair_sems, 3 * self.count + k, 0, True)

    def from_pair(self, da):
        group = {0: 0, self.p.side - 1: 1, 1: 2, 2: 3}[da]
        for k in range(self.count):
            landed(self.view(self.p.spot(da, OTHER), k), self.pair_sems[1].at[group * self.count + k])


class ColumnGather:
    def __init__(self, place, sends, buf, up, down, far):
        self.p, self.sends, self.buf = place, sends, buf
        self.up, self.down, self.far_sems = up, down, far
        self.order = [(0, SAME)] + rel_order(place.side)

    def go(self, line, k, sems, db):
        v = self.buf.at[line, self.p.spot(*self.order[k])]
        self.sends(v, v, sems[0].at[k], sems[1].at[k], self.p.above(db), lambda: (self.buf.at[0, 0], sems[0].at[k]))

    def own(self, k):
        self.go(self.p.b, k, self.up, 1)
        self.go(self.p.b, k, self.down, self.p.side - 1)

    def near(self, k):
        p, back = self.p, self.p.side - 1
        spot = p.spot(*self.order[k])
        landed(self.buf.at[p.line(back), spot], self.up[1].at[k])
        if k % 2 == 0:
            self.go(p.line(back), k, self.far_sems, 1)
        landed(self.buf.at[p.line(1), spot], self.down[1].at[k])
        if k % 2 == 1:
            self.go(p.line(1), k, self.far_sems, back)

    def far(self, k):
        landed(self.buf.at[self.p.line(2), self.p.spot(*self.order[k])], self.far_sems[1].at[k])


class Exchange:
    def __init__(self, place, sends, src, dst, relay, sems, hand_sems):
        self.p, self.sends, self.src, self.dst, self.relay = place, sends, src, dst, relay
        (self.s, self.r), (self.hs, self.hr, self.fs) = sems, hand_sems

    def send(self, da, other):
        p, slot = self.p, da * CORES + other
        if da == 2:
            way = p.side - 1 if other else 1
            self.sends(self.src(da, other), self.relay.at[int(other)], self.hs.at[int(other)], self.hr.at[int(other)],
                       p.mate(way))
        else:
            self.sends(self.src(da, other), self.dst(p.j), self.s.at[slot], self.r.at[p.j], p.mate(da, other))

    def hand(self):
        p, back = self.p, self.p.side - 1
        for lane, origin, way in ((0, p.spot(back), p.mate(1)), (1, p.spot(1), p.mate(back, OTHER))):
            landed(self.relay.at[lane], self.hr.at[lane])
            self.sends(self.relay.at[lane], self.dst(origin), self.fs.at[lane], self.r.at[origin], way)

    def arrived(self, da, other):
        spot = self.p.spot(da, other)
        landed(self.dst(spot), self.r.at[spot])


def dot_nt(a, b):
    return lax.dot_general(a, b, (((1,), (1,)), ((), ())), preferred_element_type=F32)


def project_kernel(side, heads, kv, w_ref, wo_ref, x_ref, cos_ref, sin_ref, na_ref, bo_ref, nr_ref, bq_ref, wr_ref,
                   k_ref, v_ref,
                   qkv_out, xb_out, pack_out, wo_out, kt_out, vt_out,
                   wl, wol, wq, xa, hh, csa, packs, acc, res, kin, vin, kmid, vmid, pass_w, pass_o, pass_x, pass_r,
                   s_wl, s_wol, s_loc, s_a2a, r_a2a, s_o, r_o, s_x, r_x, s_pk, r_pk, s_pv, r_pv,
                   s_plus, r_plus, s_minus, r_minus, s_rfar, r_rfar, s_pair, r_pair,
                   c_plus, d_plus, c_minus, d_minus, c_far, d_far, c_pair, d_pair,
                   s_up, r_up, s_dn, r_dn, s_far, r_far, s_res, r_res, s_in, s_mid,
                   h_w, h_o, h_x, h_r):
    p = Place(side)
    t = Place(side, across=True)
    row = p.row
    back = side - 1
    head = w_ref.shape[1] // (heads + 2 * kv)
    qw = heads // kv * head
    depth = w_ref.shape[0]
    wide = qw + 2 * head
    ow = wol.shape[-1]
    rel = rel_order(side)
    order = send_order(side)
    sends = Sends()

    def take(spot, dst, sem):
        parts = ((spot * qw, qw, 0), (heads * head + spot * head, head, qw),
                 ((heads + kv) * head + spot * head, head, qw + head))
        for start, size, at in parts:
            pltpu.make_async_copy(w_ref.at[:, pl.ds(pl.multiple_of(start, head), size)],
                                  dst.at[:, pl.ds(at, size)], sem).start()

    take(p.j, wq.at[p.b, p.j], s_wl.at[0])
    for k, at in enumerate(rel):
        take(p.spot(*at), wl.at[k], s_wl.at[k + 1])
    pltpu.make_async_copy(x_ref, xa.at[p.j], s_loc.at[0]).start()
    for k, at in enumerate(rel + [(0, SAME)]):
        pltpu.make_async_copy(wo_ref.at[:, pl.ds(pl.multiple_of(t.spot(*at) * ow, head), ow)], wol.at[k],
                              s_wol.at[k]).start()

    depth_in, block = kin.shape[0], kin.shape[1]
    per = k_ref.shape[1] // block
    steps = k_ref.shape[0] * per

    def bring(b, slot):
        r, at = b // per, lax.rem(b, per) * block
        return (pltpu.make_async_copy(k_ref.at[r, pl.ds(at, block)], kin.at[slot], s_in.at[slot]),
                pltpu.make_async_copy(v_ref.at[r, pl.ds(at, block)], vin.at[slot], s_in.at[depth_in + slot]))

    def put(b, slot):
        r, at = b // per, lax.rem(b, per) * block
        return (pltpu.make_async_copy(kmid.at[slot], kt_out.at[r, :, pl.ds(at, block)], s_mid.at[slot]),
                pltpu.make_async_copy(vmid.at[slot], vt_out.at[r, :, pl.ds(at, block)], s_mid.at[depth_in + slot]))

    def turn(b, _):
        slot = lax.rem(b, depth_in)
        for copy in bring(b, slot):
            copy.wait()

        @pl.when(b >= depth_in)
        def _():
            for copy in put(b - depth_in, slot):
                copy.wait()
        kmid[slot] = pltpu.einshape('skd->ksd', kin[slot])
        vmid[slot] = pltpu.einshape('skd->ksd', vin[slot])
        for copy in put(b, slot):
            copy.start()

        @pl.when(b + depth_in < steps)
        def _():
            for copy in bring(b + depth_in, slot):
                copy.start()
        return 0

    done = [0]

    def fill(n):
        n = min(n, steps - done[0])
        if n > 0:
            lax.fori_loop(done[0], done[0] + n, turn, 0)
            done[0] += n

    for b in range(depth_in):
        for copy in bring(b, b):
            copy.start()
    packs[p.b, p.j] = jnp.concatenate(
        [na_ref[...].astype(F32), bo_ref[...].astype(F32), nr_ref[...].astype(F32), bq_ref[...],
         jnp.zeros((2, head), F32), wr_ref[...].astype(F32)], axis=0)
    csa[p.j] = jnp.concatenate([cos_ref[...], sin_ref[...]], axis=-1)

    meet(p.mates() + [t.mate(da, other) for da in range(1, side) for other in BOTH])

    gather = ColumnGather(p, sends, wq, (s_up, r_up), (s_dn, r_dn), (s_far, r_far))
    count = r_plus.shape[0]
    cut = xa.shape[1] // count
    tokens = RowGather(p, sends, lambda spot, k: xa.at[spot, pl.ds(k * cut, cut)], count,
                       (s_plus, r_plus), (s_minus, r_minus), (s_rfar, r_rfar), (s_pair, r_pair))
    turns = d_plus.shape[0]
    cut_cs = csa.shape[1] // turns
    tables = RowGather(p, sends, lambda spot, k: csa.at[spot, pl.ds(k * cut_cs, cut_cs)], turns,
                       (c_plus, d_plus), (c_minus, d_minus), (c_far, d_far), (c_pair, d_pair))
    swap_w = Exchange(p, sends, lambda da, other: wl.at[rel.index((da, other))], lambda spot: wq.at[p.b, spot], pass_w,
                      (s_a2a, r_a2a), (h_w.at[0], h_w.at[1], h_w.at[2]))
    swap_o = Exchange(t, sends, lambda da, other: wol.at[rel.index((da, other))], lambda spot: wo_out.at[spot], pass_o,
                      (s_o, r_o), (h_o.at[0], h_o.at[1], h_o.at[2]))
    swap_x = Exchange(
        t, sends, lambda da, other: xa.at[p.j, :, pl.ds(pl.multiple_of(t.spot(da, other) * ow, head), ow)],
        lambda spot: xb_out.at[spot], pass_x, (s_x, r_x), (h_x.at[0], h_x.at[1], h_x.at[2]))
    swap_r = Exchange(
        p, sends, lambda da, other: res.at[da * CORES + (1 - p.c if other else p.c)],
        lambda spot: qkv_out.at[spot], pass_r, (s_res, r_res), (h_r.at[0], h_r.at[1], h_r.at[2]))
    landed(wq.at[p.b, p.j], s_wl.at[0])
    gather.own(0)
    mine = packs.at[p.b, p.j]
    for k, at in enumerate(rel):
        sends(mine, mine, s_pk.at[k], r_pk.at[p.j], p.mate(*at))
    for at in order:
        landed(wl.at[rel.index(at)], s_wl.at[rel.index(at) + 1])
        swap_w.send(*at)
    for k in range(turns):
        tables.own(k)
    landed(xa.at[p.j], s_loc.at[0])
    tokens.own(0)

    for at in rel:
        landed(packs.at[p.b, p.spot(*at)], r_pk.at[p.spot(*at)])
    pv = packs.at[p.b]
    sends(pv, pv, s_pv.at[0], r_pv.at[0], p.above(1))
    sends(pv, pv, s_pv.at[1], r_pv.at[1], p.above(back))
    for k, at in enumerate(rel):
        swap_w.arrived(*at)
        gather.own(k + 1)
        if k == 0:
            pu = packs.at[p.line(back)]
            landed(pu, r_pv.at[0])
            sends(pu, pu, s_pv.at[2], r_pv.at[2], p.above(1))
        if k == 2:
            swap_w.hand()
            for i in range(1, count):
                tokens.own(i)
        fill(2)
    landed(packs.at[p.line(1)], r_pv.at[1])
    landed(packs.at[p.line(2)], r_pv.at[2])
    for k in range(turns):
        tables.near(k)
    out_pack = pltpu.make_async_copy(packs, pack_out, s_loc.at[2])
    out_pack.start()

    model = xa.shape[-1]

    def norm(spot):
        total = jnp.zeros((xa.shape[1], head), F32)
        for i in range(model // head):
            v = xa[spot, :, i * head:(i + 1) * head].astype(F32)
            total = total + v * v
        inv = lax.rsqrt(jnp.sum(total, axis=-1, keepdims=True) / model + NORM_EPS)
        for i in range(model // head):
            v = xa[spot, :, i * head:(i + 1) * head].astype(F32)
            g = packs[i // row, i % row, 0:1, :]
            hh[spot, :, i * head:(i + 1) * head] = (v * inv * g).astype(BF16)

    span = row * depth

    def part(da, db):
        chip = lax.rem(p.a + da, side)
        rows = hh[pl.ds(chip * CORES, CORES), :, pl.ds(pl.multiple_of(p.line(db) * span, span), span)]
        rows = rows.reshape(CORES * hh.shape[1], span)
        return jnp.dot(rows, wq[p.line(db)].reshape(span, wide), preferred_element_type=F32)

    def bias(m):
        e, k = m // 3, lax.rem(m, 3)
        out = 0.0
        for c in range(CORES):
            d = e * CORES + c
            out = out + packs[d // row, lax.rem(d, row), pl.ds(3 + k, 1), :]
        return out

    lanes = lax.broadcasted_iota(jnp.int32, (1, head), 1)

    def finish(da):
        total = acc[da] + part(da, 2)
        chip = lax.rem(p.a + da, side)
        cs = csa[pl.ds(chip * CORES, CORES)].reshape(CORES * csa.shape[1], head)
        turned = pltpu.roll(cs, head // 2, 1)
        low = lanes < head // 2
        cos = jnp.where(low, cs, turned)
        sin = jnp.where(low, -turned, cs)
        n_q = heads // kv
        for i in range(n_q + 2):
            m = p.j * n_q + i if i < n_q else (heads + p.j if i == n_q else heads + kv + p.j)
            v = total[:, i * head:(i + 1) * head] + bias(m)
            if i <= n_q:
                v = v * cos + pltpu.roll(v, head // 2, 1) * sin
            res[da * CORES:(da + 1) * CORES, :, i * head:(i + 1) * head] = v.astype(BF16).reshape(CORES, -1, head)
        for other in BOTH:
            if da or other:
                swap_r.send(da, other)
        if not da:
            pltpu.make_async_copy(res.at[p.c], qkv_out.at[p.j], r_res.at[p.j]).start()

    norm(p.spot(0))
    tokens.from_pair(0)
    norm(p.spot(0, OTHER))
    for k in range(0, 4):
        gather.near(k)
        fill(2)
    acc[0] = part(0, 0)
    for k in range(count):
        if k % 2 == 0:
            for i in range(4 + k, 4 + k + 2):
                gather.near(i)
            fill(2)
        tokens.near(k)
        fill(2)
    for at in order:
        landed(wol.at[rel.index(at)], s_wol.at[rel.index(at)])
        swap_o.send(*at)
    for at in order:
        swap_x.send(*at)
    for k in range(turns):
        tables.far(k)
    landed(wol.at[row - 1], s_wol.at[row - 1])
    own_o = pltpu.make_async_copy(wol.at[row - 1], wo_out.at[t.j], s_loc.at[1])
    own_o.start()
    own_x = pltpu.make_async_copy(xa.at[p.j, :, pl.ds(pl.multiple_of(t.j * ow, head), ow)], xb_out.at[t.j], s_loc.at[3])
    own_x.start()
    fill(steps)
    acc[0] += part(0, 1)
    acc[0] += part(0, back)
    for da in (back, 1):
        norm(p.spot(da))
        tokens.from_pair(da)
        norm(p.spot(da, OTHER))
        acc[da] = part(da, 0)
        acc[da] += part(da, 1)
        acc[da] += part(da, back)
    for da in range(side):
        tables.from_pair(da)
    for k in range(count // 2):
        tokens.far(k)
    for k in range(row):
        gather.far(k)
    finish(1)
    finish(back)
    for k in range(count // 2, count):
        tokens.far(k)
    norm(p.spot(2))
    tokens.from_pair(2)
    norm(p.spot(2, OTHER))
    acc[2] = part(2, 0)
    acc[2] += part(2, 1)
    acc[2] += part(2, back)
    finish(2)
    swap_o.hand()
    finish(0)
    swap_x.hand()
    swap_r.hand()
    for at in rel:
        swap_o.arrived(*at)
        swap_x.arrived(*at)
    for b in range(steps - depth_in, steps):
        for copy in put(b, b % depth_in):
            copy.wait()
    for i in range(row):
        landed(qkv_out.at[i], r_res.at[i])
    own_o.wait()
    own_x.wait()
    out_pack.wait()
    sends.finish()


def output_kernel(side, kv, len_ref, sink_ref, qkv_ref, kt_ref, vt_ref, wo_ref, xb_ref, packs, own,
                  kb, vb, sb0, sb1, mb0, mb1, lb0, lb1, oa, wq, xbv, acc, res, pass_r,
                  s_k, s_v, s_loc, s_plus, r_plus, s_minus, r_minus, s_rfar, r_rfar, s_pair, r_pair,
                  s_up, r_up, s_dn, r_dn, s_far, r_far, s_res, r_res, h_r):
    p = Place(side, across=True)
    row = p.row
    back = side - 1
    head = packs.shape[-1]
    depth = wq.shape[2]
    wide = wq.shape[3]
    n_tok = oa.shape[1]
    n_req = kt_ref.shape[0]
    slots = kt_ref.shape[2]
    new = n_tok // n_req
    group = qkv_ref.shape[2] // head - 2
    rows = group * new
    total = n_req * kv
    scale = head ** -0.5 * LOG2E
    block = min(512, slots)
    sends = Sends()
    loads = [pltpu.make_async_copy(wo_ref, wq.at[p.b], s_loc.at[0]),
             pltpu.make_async_copy(xb_ref, xbv, s_loc.at[1])]
    for copy in loads:
        copy.start()

    deep = kb.shape[0]
    quarter = slots // deep

    def fetch(n, which, buf, sem):
        slot = lax.rem(n, deep)

        @pl.when(n < total)
        def _():
            for k in range(deep):
                at = pl.ds(k * quarter, quarter)
                pltpu.make_async_copy(which.at[n // kv, lax.rem(n, kv), at], buf.at[slot, at], sem.at[slot]).start()

    def fetched(n, buf, sem):
        slot = lax.rem(n, deep)

        @pl.when(n < total)
        def _():
            landed(buf.at[slot], sem.at[slot])

    for n in range(deep):
        fetch(jnp.int32(n), kt_ref, kb, s_k)
        fetch(jnp.int32(n), vt_ref, vb, s_v)
    meet(p.mates() + [p.above(1), p.above(back)])
    gather = ColumnGather(p, sends, wq, (s_up, r_up), (s_dn, r_dn), (s_far, r_far))
    count = r_plus.shape[0]
    cuts = count // n_req
    lanes = row * wide // cuts
    tokens = RowGather(
        p, sends, lambda spot, k: oa.at[spot, pl.ds(k // cuts * new, new), pl.ds(k % cuts * lanes, lanes)], count,
        (s_plus, r_plus), (s_minus, r_minus), (s_rfar, r_rfar), (s_pair, r_pair))
    swap_r = Exchange(
        p, sends, lambda da, other: res.at[da * CORES + (1 - p.c if other else p.c)],
        lambda spot: own.at[spot], pass_r, (s_res, r_res), (h_r.at[0], h_r.at[1], h_r.at[2]))
    loads[0].wait()
    for k in range(row):
        gather.own(k)
    loads[1].wait()

    def place(r):
        return pl.ds(pl.multiple_of(r * new, new), new)

    ri = lax.rem(lax.broadcasted_iota(jnp.int32, (rows, head), 0), new)
    ci = lax.broadcasted_iota(jnp.int32, (rows, head), 1)

    def first(n, sb, mb, lb):
        slot = lax.rem(n, deep)
        n = jnp.minimum(n, total - 1)
        r, i = n // kv, lax.rem(n, kv)
        q = jnp.concatenate([qkv_ref[i, place(r), g * head:(g + 1) * head] for g in range(group)], axis=0)
        length = len_ref[r]
        kn = qkv_ref[i, place(r), group * head:(group + 1) * head]
        kn = jnp.concatenate([kn, jnp.zeros((head - new, head), BF16)], axis=0)
        s = jnp.where(ri >= ci, dot_nt(q, kn), -1e30)
        sb[:, slots:] = s
        m = s
        for b in range(slots // block):
            s = dot_nt(q, kb[slot, b * block:(b + 1) * block])
            s = jnp.where(b * block + lax.broadcasted_iota(jnp.int32, (1, block), 1) < length, s, -1e30)
            sb[:, b * block:(b + 1) * block] = s
            for k in range(block // head):
                m = jnp.maximum(m, s[:, k * head:(k + 1) * head])
            yield
        m = jnp.max(m, axis=-1, keepdims=True) * scale
        sink = jnp.concatenate([jnp.full((new, head), sink_ref[i * group + g] * LOG2E, F32) for g in range(group)], axis=0)
        m = jnp.maximum(m, sink)
        mb[...] = m
        lb[...] = jnp.exp2(sink - m)

    def second(n, sb, mb, lb):
        slot = lax.rem(n, deep)
        r, i = n // kv, lax.rem(n, kv)
        m = mb[...]
        vn = qkv_ref[i, place(r), (group + 1) * head:]
        vn = jnp.concatenate([vn, jnp.zeros((head - new, head), BF16)], axis=0)
        pr = jnp.exp2(sb[:, slots:] * scale - m)
        low = pr
        out = jnp.dot(pr.astype(BF16), vn, preferred_element_type=F32)
        for b in range(slots // block):
            prs = []
            for k in range(block // head):
                at = b * block + k * head
                pr = jnp.exp2(sb[:, at:at + head] * scale - m)
                low = low + pr
                prs.append(pr.astype(BF16))
            out = out + jnp.dot(jnp.concatenate(prs, axis=1), vb[slot, b * block:(b + 1) * block], preferred_element_type=F32)
            yield
        out = (out / (jnp.sum(low, axis=-1, keepdims=True) + lb[...])).astype(BF16)
        for g in range(group):
            at = pl.multiple_of((i * group + g) * head, head)
            oa[p.j, place(r), pl.ds(at, head)] = out[g * new:(g + 1) * new]

    def run(*work):
        work = list(work)
        while work:
            for w in list(work):
                if next(w, w) is w:
                    work.remove(w)

    fetched(jnp.int32(0), kb, s_k)
    run(first(jnp.int32(0), sb0, mb0, lb0))
    fetch(jnp.int32(deep), kt_ref, kb, s_k)
    turns = total // 2
    each = turns // count

    def events(h):
        out = []
        if (h + 1) % each == 0:
            out.append((tokens.own, h // each))
        for k in range(count):
            if h == (k + 1) * each + 2:
                out.append((tokens.near, k))
            if h == (k + 1) * each + 5:
                out.append((tokens.far, k))
        if h >= turns // 2:
            for k in range(row):
                if turns // 2 + k // 2 == h:
                    out.append((gather.near, k))
        return out

    def body(h, _):
        for n, one, two in ((2 * h, (sb1, mb1, lb1), (sb0, mb0, lb0)), (2 * h + 1, (sb0, mb0, lb0), (sb1, mb1, lb1))):
            fetched(n, vb, s_v)
            fetched(n + 1, kb, s_k)
            run(first(n + 1, *one), second(n, *two))
            fetch(n + deep, vt_ref, vb, s_v)
            fetch(n + deep + 1, kt_ref, kb, s_k)
        for at in range(turns):
            todo = events(at)
            if todo:
                @pl.when(h == at)
                def _():
                    for act, k in todo:
                        act(k)
        return 0

    lax.fori_loop(0, turns, body, 0)
    past = [e for h in range(turns) for e in events(h)]

    def rest(act, k):
        if not any(a == act and i == k for a, i in past):
            act(k)

    def part(da, db):
        chip = lax.rem(p.a + da, side)
        cols = [oa[pl.ds(chip * CORES, CORES), :, pl.ds(pl.multiple_of(p.device(a, p.line(db), 0) * depth, depth), CORES * depth)]
                for a in range(side)]
        lhs = jnp.concatenate([v.reshape(CORES * n_tok, CORES * depth) for v in cols], axis=-1)
        return jnp.dot(lhs, wq[p.line(db)].reshape(row * depth, wide), preferred_element_type=F32)

    def finish(da):
        total = acc[da] + part(da, 2)
        chip = lax.rem(p.a + da, side)
        for i in range(wide // head):
            d = p.j * (wide // head) + i
            b = packs[d // row, lax.rem(d, row), 1:2, :]
            at = pl.ds(i * head, head)
            base = xbv[pl.ds(chip * CORES, CORES), :, at].reshape(-1, head).astype(F32)
            v = base + (total[:, i * head:(i + 1) * head] + b)
            res[da * CORES:(da + 1) * CORES, :, at] = v.astype(BF16).reshape(CORES, -1, head)
        for other in BOTH:
            if da or other:
                swap_r.send(da, other)
        if not da:
            pltpu.make_async_copy(res.at[p.c], own.at[p.j], r_res.at[p.j]).start()

    for k in range(row):
        rest(gather.near, k)
    for k in range(count):
        rest(tokens.near, k)
    for k in range(count // 2):
        rest(tokens.far, k)
    for da in (back, 1):
        tokens.from_pair(da)
        acc[da] = part(da, 0)
        acc[da] += part(da, 1)
        acc[da] += part(da, back)
    for k in range(row):
        gather.far(k)
    finish(1)
    finish(back)
    for k in range(count // 2, count):
        rest(tokens.far, k)
    tokens.from_pair(2)
    acc[2] = part(2, 0)
    acc[2] += part(2, 1)
    acc[2] += part(2, back)
    finish(2)
    tokens.from_pair(0)
    acc[0] = part(0, 0)
    acc[0] += part(0, 1)
    acc[0] += part(0, back)
    finish(0)
    swap_r.hand()
    for i in range(row):
        landed(own.at[i], r_res.at[i])
    sends.finish()


def close_kernel(own, qkv_ref, packs, br_ref, resid_out, logit_out, k_out, v_out):
    row, n_tok, wide = own.shape
    n_req, experts, new = logit_out.shape
    head = packs.shape[-1]
    model = row * wide
    for r in range(n_req):
        k_out[r] = pltpu.einshape('jtd->tjd', qkv_ref[:, r * new:(r + 1) * new, :head])
        v_out[r] = pltpu.einshape('jtd->tjd', qkv_ref[:, r * new:(r + 1) * new, head:])
    square = jnp.zeros((n_tok, head), F32)
    for i in range(row):
        resid_out[:, i * wide:(i + 1) * wide] = own[i]
        for k in range(wide // head):
            v = own[i, :, k * head:(k + 1) * head].astype(F32)
            square = square + v * v
    inv = lax.rsqrt(jnp.sum(square, axis=-1, keepdims=True) / model + NORM_EPS)
    logits = jnp.zeros((experts, n_tok), F32)
    for i in range(row):
        for k in range(wide // head):
            d = i * (wide // head) + k
            v = own[i, :, k * head:(k + 1) * head].astype(F32)
            g = (v * inv * packs[d // row, d % row, 2:3, :]).astype(BF16)
            w = packs[d // row, d % row, 8:8 + experts, :].astype(BF16)
            logits = logits + dot_nt(w, g)
    logits = logits + br_ref[...]
    for r in range(n_req):
        logit_out[r] = logits[:, r * new:(r + 1) * new]


def dma(*shape):
    return pltpu.SemaphoreType.DMA(shape)


def solution(mesh):
    row_spec = P(('dp', 'fsdp'))
    shard_spec = P('fsdp')
    whole_spec = P()
    n_dev = mesh.shape[AXIS]
    side = math.isqrt(n_dev // CORES)
    row = side * CORES
    hbm = pl.BlockSpec(memory_space=pl.ANY)
    vmem = pl.BlockSpec(memory_space=pltpu.VMEM)
    smem = pl.BlockSpec(memory_space=pltpu.SMEM)

    def local_step(tokens, k_cache, v_cache, prefix_len, rope_cos, rope_sin, norm_attn, w_qkv, b_qkv, sink_logits, w_out, b_out, norm_router, w_router, b_router):
        n_req, n_new, model = tokens.shape
        kv, head = k_cache.shape[2:]
        heads = sink_logits.shape[0]
        experts = b_router.shape[0]
        depth = w_qkv.shape[0]
        n_tok = n_req * n_new
        wide = w_qkv.shape[1] // row
        ow = model // row
        flat = tokens.reshape(n_tok, model)
        core = lax.rem(lax.axis_index(AXIS), CORES)
        bias_pad = lax.dynamic_update_slice(jnp.zeros((3 * head,), F32), b_qkv.astype(F32), (core * b_qkv.shape[0],))
        n_pack = 8 + experts

        pieces = 4
        turn = 256
        slots = k_cache.shape[1]
        qkv, xb, packs, wo, kt, vt = pl.pallas_call(
            functools.partial(project_kernel, side, heads, kv),
            out_shape=(jax.ShapeDtypeStruct((row, n_tok, wide), BF16),
                       jax.ShapeDtypeStruct((row, n_tok, ow), BF16),
                       jax.ShapeDtypeStruct((side, row, n_pack, head), F32),
                       jax.ShapeDtypeStruct((row, depth, ow), BF16),
                       jax.ShapeDtypeStruct((n_req, kv, slots, head), BF16),
                       jax.ShapeDtypeStruct((n_req, kv, slots, head), BF16)),
            in_specs=[hbm, hbm, hbm] + [vmem] * 7 + [hbm, hbm],
            out_specs=(hbm,) * 6,
            scratch_shapes=[
                pltpu.VMEM((row - 1, depth, wide), BF16),
                pltpu.VMEM((row, depth, ow), BF16),
                pltpu.VMEM((side, row, depth, wide), BF16),
                pltpu.VMEM((row, n_tok, model), BF16),
                pltpu.VMEM((row, n_tok, model), BF16),
                pltpu.VMEM((row, n_tok, head), F32),
                pltpu.VMEM((side, row, n_pack, head), F32),
                pltpu.VMEM((side, CORES * n_tok, wide), F32),
                pltpu.VMEM((row, n_tok, wide), BF16),
                *[pltpu.VMEM((pieces, turn, kv, head), BF16)] * 2, *[pltpu.VMEM((pieces, kv, turn, head), BF16)] * 2,
                pltpu.VMEM((2, depth, wide), BF16), *[pltpu.VMEM((2, depth, ow), BF16)] * 2,
                pltpu.VMEM((2, n_tok, wide), BF16),
                *[dma(row)] * 2, dma(pieces), *[dma(row)] * 8, *[dma(side)] * 2,
                *[dma(pieces)] * 6, *[dma(side * pieces)] * 2, *[dma(2)] * 6, *[dma(2 * side)] * 2,
                *[dma(row)] * 8, *[dma(2 * pieces)] * 2, *[dma(3, 2)] * 4],
            compiler_params=pltpu.CompilerParams(collective_id=0, has_side_effects=True, vmem_limit_bytes=60 * 2**20),
            name='project',
        )(w_qkv, w_out, flat, rope_cos.reshape(n_tok, head // 2), rope_sin.reshape(n_tok, head // 2),
          norm_attn.reshape(1, head), b_out.reshape(1, head), norm_router.reshape(1, head),
          bias_pad.reshape(3, head), w_router.T, k_cache, v_cache)

        n_row = heads // kv * n_new
        parts = 4 * n_req
        own = pl.pallas_call(
            functools.partial(output_kernel, side, kv),
            out_shape=jax.ShapeDtypeStruct((row, n_tok, ow), BF16),
            in_specs=[smem, smem, vmem, hbm, hbm, hbm, hbm, vmem],
            out_specs=hbm,
            scratch_shapes=[
                *[pltpu.VMEM((4, slots, head), BF16)] * 2, *[pltpu.VMEM((n_row, slots + head), F32)] * 2,
                *[pltpu.VMEM((n_row, head), F32)] * 4,
                pltpu.VMEM((row, n_tok, model), BF16),
                pltpu.VMEM((side, row, depth, ow), BF16),
                pltpu.VMEM((row, n_tok, ow), BF16),
                pltpu.VMEM((side, CORES * n_tok, ow), F32),
                pltpu.VMEM((row, n_tok, ow), BF16),
                pltpu.VMEM((2, n_tok, ow), BF16),
                *[dma(4)] * 2, dma(2), *[dma(parts)] * 6, *[dma(side * parts)] * 2, *[dma(row)] * 8, dma(3, 2)],
            compiler_params=pltpu.CompilerParams(collective_id=1, has_side_effects=True, vmem_limit_bytes=56 * 2**20),
            name='output',
        )(prefix_len, sink_logits, qkv, kt, vt, wo, xb, packs)

        gw = wide - 2 * head
        resid, logits, k_new, v_new = pl.pallas_call(
            close_kernel,
            grid=(1,),
            out_shape=(jax.ShapeDtypeStruct((n_tok, model), BF16), jax.ShapeDtypeStruct((n_req, experts, n_new), F32),
                       jax.ShapeDtypeStruct((n_req, n_new, kv, head), BF16),
                       jax.ShapeDtypeStruct((n_req, n_new, kv, head), BF16)),
            in_specs=[pl.BlockSpec((row, n_tok, ow), lambda i: (0, 0, 0)),
                      pl.BlockSpec((row, n_tok, 2 * head), lambda i: (0, 0, gw // (2 * head))),
                      pl.BlockSpec((side, row, n_pack, head), lambda i: (0, 0, 0, 0)),
                      pl.BlockSpec((experts, 1), lambda i: (0, 0))],
            out_specs=(pl.BlockSpec((n_tok, model), lambda i: (0, 0)), pl.BlockSpec((n_req, experts, n_new), lambda i: (0, 0, 0)),
                       pl.BlockSpec((n_req, n_new, kv, head), lambda i: (0, 0, 0, 0)),
                       pl.BlockSpec((n_req, n_new, kv, head), lambda i: (0, 0, 0, 0))),
            name='close',
        )(own, qkv, packs, b_router.reshape(experts, 1))
        return (resid.reshape(n_req, n_new, model), jnp.transpose(logits, (0, 2, 1)), k_new, v_new)

    in_specs = (row_spec, row_spec, row_spec, row_spec, row_spec, row_spec, shard_spec, shard_spec, shard_spec, whole_spec, shard_spec, shard_spec, shard_spec, shard_spec, whole_spec)
    out_specs = (row_spec, row_spec, row_spec, row_spec)
    return jax.shard_map(local_step, mesh=mesh, in_specs=in_specs, out_specs=out_specs, check_vma=False)
```
